256 devices in a mesh: seq: 32 (over x, z_lo, core), head: 8 (over y, z_hi).
Axes of the slice: x: 4, y: 4, z: 8 (z_hi: 2, z_lo: 4; z = z_hi * 4 + z_lo), core: 2. Of those that a mesh axis runs over, the one named last changes fastest.
Arguments:
- tokens: bfloat16 [16384, 1024], P('seq'), may hold values from -6 to 6
- mem_query_w: bfloat16 [1024, 1024], P(None, 'head'), may hold values from -0.1875 to 0.1875
- mem_key_w: bfloat16 [1024, 1024], P(None, 'head'), may hold values from -0.1875 to 0.1875
- mem_value_w: bfloat16 [1024, 1024], P(None, 'head'), may hold values from -0.1875 to 0.1875
- mem_in: float32 [1024, 1024], P(None, 'head'), may hold values from -0.1875 to 0.1875
- mem_out: float32 [1024, 1024], P('head'), may hold values from -0.1875 to 0.1875
- forget_levels: float32 [16, 1024], P(None, 'head'), may hold values from 0.003 to 0.3
- momentum_levels: float32 [16, 1024], P(None, 'head'), may hold values from 0.2 to 0.9
- step_levels: float32 [16, 1024], P(None, 'head'), may hold values from 0.02 to 0.2
- plan: int32 [32], P('seq'), may hold values from 0 to 15
- norm_gain: float32 [1024], replicated, may hold values from 0.5 to 1.5
- attn_query_w: bfloat16 [1024, 1024], P(None, 'head'), may hold values from -1 to 1
- attn_key_w: bfloat16 [1024, 1024], P(None, 'head'), may hold values from -4 to 4
- attn_value_w: bfloat16 [1024, 1024], P(None, 'head'), may hold values from -0.1875 to 0.1875
- attn_out_w: bfloat16 [1024, 1024], P('head'), may hold values from -0.25 to 0.25
Outputs:
- layer_out: bfloat16 [16384, 1024], P('seq', 'head')
The draws below stay inside these ranges and needn't reach their ends.
All inputs are finite; a program needn't handle non-finite values.
Results may differ from the reference program's by a relative error of at most 0.014.
Values may be sent and summed in bfloat16 or wider, within the bound.
A program may use at most 128 MiB of HBM per device.

```python
import math
import jax
import jax.numpy as jnp
from jax import lax

D = 1024
HEAD_DIM = 64
MEM_HID = 1024
LEVELS = 16
SPAN = 8
TOK_DEV = 512
GROUPS = 32
LENGTH = 16384


def attention_pair(key):
    shared = jax.random.normal(jax.random.fold_in(key, 11), (D, D), jnp.float32) / math.sqrt(D)
    others = jax.random.normal(jax.random.fold_in(key, 12), (D, D), jnp.float32) / math.sqrt(D)
    return (shared, others)


def draw_attn_query_w(key, part):
    shared, others = attention_pair(key)
    return jnp.clip(shared, -1.0, 1.0).astype(jnp.bfloat16)


def draw_attn_key_w(key, part):
    shared, others = attention_pair(key)
    return jnp.clip(others, -4.0, 4.0).astype(jnp.bfloat16)


def touch_ends(array, key, smallest, largest):
    extent = array.shape
    spot = [jax.random.randint(jax.random.fold_in(key, axis), (), 0, extent[axis]) for axis in range(len(extent))]
    array = array.at[tuple(spot)].set(smallest)
    longest = extent.index(max(extent))
    spot[longest] = (spot[longest] + 1) % extent[longest]
    return array.at[tuple(spot)].set(largest)


def spiked(drawn, stream_key, source, target, shards_of, factor):
    def block_of(position):
        return (jnp.arange(drawn.shape[position]) // (drawn.shape[position] // shards_of)).reshape((-1,) + (1,) * (drawn.ndim - 1 - position))

    near = jax.random.permutation(stream_key, shards_of)[block_of(target)]
    far = (block_of(target) + shards_of // 2) % shards_of
    return jnp.where((block_of(source) == near) | (block_of(source) == far), factor * drawn, drawn)


def shard_levels(own_key, extent, split, least, largest):
    factor_of = 1.0
    for position, shards_of in split:
        steps = jax.random.uniform(jax.random.fold_in(jax.random.fold_in(own_key, 6), position), (shards_of,), jnp.float32, least / len(split), largest / len(split))
        factor_of = factor_of * jnp.repeat(jnp.exp(steps), extent[position] // shards_of).reshape((-1,) + (1,) * (len(extent) - 1 - position))
    return factor_of


def scatter_about(rng, extent, spread, most, split=(), kind=jnp.bfloat16):
    factor_of = shard_levels(rng, extent, split, -0.22, 0.18) if split else 1.0
    result = jax.random.normal(rng, extent, jnp.float32) * spread * factor_of
    return jnp.minimum(jnp.maximum(result, -most), most).astype(kind)


def heavy_noise(own_key, dims, width, limit, shards, heavy, kind=jnp.bfloat16):
    result = width * jax.random.normal(own_key, dims, jnp.float32)
    if shards:
        result = result * shard_levels(own_key, dims, shards, -0.22, 0.18)
    return jnp.clip(spiked(result, jax.random.fold_in(own_key, 3), *heavy), -limit, limit).astype(kind)


def setup_inputs(seed: int = 0) -> dict:
    splits = jax.random.split(jax.random.key(seed), 16)
    tokens = scatter_about(splits[0], (LENGTH, D), 1.0, 6.0, ((0, 32),))
    mem_query_w = scatter_about(splits[1], (D, D), D ** -0.5, 0.1875, ((1, 8),))
    mem_key_w = scatter_about(splits[2], (D, D), D ** -0.5, 0.1875, ((1, 8),))
    mem_value_w = scatter_about(splits[3], (D, D), D ** -0.5, 0.1875, ((1, 8),))
    mem_in = scatter_about(splits[4], (D, MEM_HID), D ** -0.5, 0.1875, ((1, 8),), jnp.float32)
    mem_out = scatter_about(splits[5], (MEM_HID, D), MEM_HID ** -0.5, 0.1875, ((0, 8),), jnp.float32)
    forget_levels = jnp.clip(jnp.exp(math.log(0.3) - 4.6051702 * jax.random.uniform(splits[6], (LEVELS, MEM_HID), jnp.float32) ** shard_levels(splits[6], (LEVELS, MEM_HID), ((1, 8),), -0.2, 0.2)), 0.003, 0.3)
    momentum_levels = jnp.clip(0.2 + 0.7 * jax.random.uniform(splits[7], (LEVELS, MEM_HID), jnp.float32) ** shard_levels(splits[7], (LEVELS, MEM_HID), ((1, 8),), -0.2, 0.2), 0.2, 0.9)
    step_levels = jnp.clip(jnp.exp(math.log(0.2) - 2.3025851 * jax.random.uniform(splits[8], (LEVELS, MEM_HID), jnp.float32) ** shard_levels(splits[8], (LEVELS, MEM_HID), ((1, 8),), -0.2, 0.2)), 0.02, 0.2)
    plan = touch_ends(jax.random.randint(splits[9], (GROUPS,), 0, LEVELS), jax.random.fold_in(splits[9], 1), 0, LEVELS - 1).astype(jnp.int32)
    norm_gain = jnp.clip(1.0 + 0.1 * jax.random.normal(splits[10], (D,), jnp.float32), 0.5, 1.5)
    attn_query_w = draw_attn_query_w(jax.random.fold_in(splits[15], 71), 0)
    attn_key_w = draw_attn_key_w(jax.random.fold_in(splits[15], 71), 0)
    attn_value_w = scatter_about(splits[13], (D, D), D ** -0.5, 0.1875, ((1, 8),))
    attn_out_w = heavy_noise(splits[14], (D, D), D ** -0.5, 0.25, ((0, 8),), (0, 1, 8, 2.0))
    return {"tokens": tokens, "mem_query_w": mem_query_w, "mem_key_w": mem_key_w, "mem_value_w": mem_value_w, "mem_in": mem_in, "mem_out": mem_out, "forget_levels": forget_levels, "momentum_levels": momentum_levels, "step_levels": step_levels, "plan": plan, "norm_gain": norm_gain, "attn_query_w": attn_query_w, "attn_key_w": attn_key_w, "attn_value_w": attn_value_w, "attn_out_w": attn_out_w}


highest = lax.Precision.HIGHEST
epsilon = 1e-06

def silu_slope(values):
    sigmoid = jax.nn.sigmoid(values)
    return sigmoid * (1.0 + values * (1.0 - sigmoid))

def project(left, weight):
    return jnp.dot(left, weight, preferred_element_type=jnp.float32).astype(jnp.bfloat16)

def normalize(retrieved, norm_gain):
    mean_square = lax.optimization_barrier(jnp.mean(retrieved * retrieved, axis=-1, keepdims=True))
    return (retrieved * lax.rsqrt(mean_square + epsilon) * norm_gain).astype(jnp.bfloat16)

def window_attend(query, keys, values, block_index, head_dim):
    query_count = query.shape[0]
    key_count = keys.shape[0]
    head_count = query.shape[1] // head_dim
    query_heads = query.reshape(query_count, head_count, head_dim).astype(jnp.float32)
    key_heads = keys.reshape(key_count, head_count, head_dim).astype(jnp.float32)
    value_heads = values.reshape(key_count, head_count, head_dim).astype(jnp.float32)
    scores = jnp.einsum('qhd,khd->hqk', query_heads, key_heads) * head_dim ** (-0.5)
    span_rows = key_count - query_count
    distance = span_rows + jnp.arange(query_count, dtype=jnp.int32)[:, None] - jnp.arange(key_count, dtype=jnp.int32)[None, :]
    key_pos = (block_index * query_count - span_rows + jnp.arange(key_count, dtype=jnp.int32))[None, :]
    allowed = (distance >= 0) & (distance < span_rows) & (key_pos >= 0)
    scores = jnp.where(allowed[None], scores, -1e+30)
    row_peak = lax.optimization_barrier(jnp.max(scores, axis=-1, keepdims=True))
    weights = jnp.exp(scores - row_peak)
    probabilities = (weights / lax.optimization_barrier(jnp.sum(weights, axis=-1, keepdims=True))).astype(jnp.bfloat16)
    context = jnp.einsum('hqk,khd->qhd', probabilities.astype(jnp.float32), value_heads)
    return context.reshape(query_count, head_count * head_dim).astype(jnp.bfloat16)

def reference(tokens, mem_query_w, mem_key_w, mem_value_w, mem_in, mem_out, forget_levels, momentum_levels, step_levels, plan, norm_gain, attn_query_w, attn_key_w, attn_value_w, attn_out_w):
    mem_query = project(tokens, mem_query_w).reshape(GROUPS, TOK_DEV, D)
    mem_key = project(tokens, mem_key_w).reshape(GROUPS, TOK_DEV, D)
    mem_value = project(tokens, mem_value_w).reshape(GROUPS, TOK_DEV, D)

    def group_step(state_now, inputs):
        speed_in, speed_out, weight_in, weight_out = state_now
        query_rows, key_rows, value_rows, chosen = inputs
        keys_wide = key_rows.astype(jnp.float32)
        pre_act = jnp.dot(keys_wide, mem_in, precision=highest)
        hidden = jax.nn.silu(pre_act)
        predicted = jnp.dot(hidden, mem_out, precision=highest)
        residual_err = 2.0 / TOK_DEV * (predicted - value_rows.astype(jnp.float32))
        grad_out = jnp.dot(hidden.T, residual_err, precision=highest)
        slope_term = jnp.dot(residual_err, mem_out.T, precision=highest) * silu_slope(pre_act)
        grad_in = jnp.dot(keys_wide.T, slope_term, precision=highest)
        query_wide = query_rows.astype(jnp.float32)
        retrieved = jnp.dot(jax.nn.silu(jnp.dot(query_wide, weight_in, precision=highest)), weight_out, precision=highest)
        forget = forget_levels[chosen]
        momentum = momentum_levels[chosen]
        step_rate = step_levels[chosen]
        speed_in = momentum[None, :] * speed_in - step_rate[None, :] * grad_in
        speed_out = momentum[:, None] * speed_out - step_rate[:, None] * grad_out
        weight_in = (1.0 - forget)[None, :] * weight_in + speed_in
        weight_out = (1.0 - forget)[:, None] * weight_out + speed_out
        return ((speed_in, speed_out, weight_in, weight_out), retrieved)
    initial = (jnp.zeros_like(mem_in), jnp.zeros_like(mem_out), mem_in, mem_out)
    last_state, retrieved = lax.scan(group_step, initial, (mem_query, mem_key, mem_value, plan))
    normed = normalize(retrieved.reshape(LENGTH, D), norm_gain)
    att_query = project(normed, attn_query_w)
    att_key = project(normed, attn_key_w)
    att_value = project(normed, attn_value_w)
    span_rows = SPAN * TOK_DEV
    padding = jnp.zeros((span_rows, D), jnp.bfloat16)
    key_padded = jnp.concatenate([padding, att_key], axis=0)
    value_padded = jnp.concatenate([padding, att_value], axis=0)

    def attend_block(block_index):
        begin = block_index * TOK_DEV
        query_block = lax.dynamic_slice_in_dim(att_query, begin, TOK_DEV, 0)
        key_block = lax.dynamic_slice_in_dim(key_padded, begin, span_rows + TOK_DEV, 0)
        value_block = lax.dynamic_slice_in_dim(value_padded, begin, span_rows + TOK_DEV, 0)
        return window_attend(query_block, key_block, value_block, block_index, HEAD_DIM)
    context = lax.map(attend_block, jnp.arange(GROUPS, dtype=jnp.int32)).reshape(LENGTH, D)
    return project(context, attn_out_w)
```

```python
import jax
import jax.numpy as jnp
from jax import lax
from jax.experimental import pallas as pl
from jax.experimental.pallas import tpu as pltpu
from jax.sharding import PartitionSpec as P

MESH = pl.DeviceIdType.MESH
F32 = jnp.float32
BF16 = jnp.bfloat16
EPS = 1e-06
NS = 32
NH = 8
T = 512
W = 128
NN = (((1,), (0,)), ((), ()))
NT = (((1,), (1,)), ((), ()))


def dot(a, b, dims=NN):
    return lax.dot_general(a, b, dims, preferred_element_type=F32)


def col(b):
    return pl.ds(pl.multiple_of(b * W, W), W)


def remote(src, dst, send, recv, device):
    return pltpu.make_async_remote_copy(
        src_ref=src, dst_ref=dst, send_sem=send, recv_sem=recv, device_id=device, device_id_type=MESH
    )


class Gather:
    def __init__(self, place, buf, send, recv):
        s, y, z = place
        self.buf, self.send, self.recv = buf, send, recv
        self.up, self.down, self.far = (y + 1) % 4, (y + 3) % 4, (y + 2) % 4
        self.s, self.y, self.z = s, y, z

    def copy(self, block, sem, yy, zz):
        ref = self.buf.at[:, col(block)]
        return remote(ref, ref, self.send.at[sem], self.recv.at[sem], (self.s, yy * 2 + zz))

    def copies(self):
        s, y, z = self.s, self.y, self.z
        o = 1 - z
        return (
            self.copy(y * 2 + z, 0, y, o),
            self.copy(y * 2 + z, 1, self.up, z),
            self.copy(y * 2 + z, 2, self.down, z),
            self.copy(y * 2 + o, 3, self.up, z),
            self.copy(y * 2 + o, 4, self.down, z),
            self.copy(self.down * 2 + z, 5, self.up, z),
            self.copy(self.up * 2 + o, 6, self.down, z),
        )

    def start(self):
        self.c = self.copies()
        for k in (1, 2, 0):
            self.c[k].start()

    def relay(self):
        self.c[1].wait_recv()
        self.c[5].start()
        self.c[0].wait_recv()
        self.c[3].start()
        self.c[4].start()
        self.c[4].wait_recv()
        self.c[6].start()

    def finish(self):
        for k in (2, 3, 5, 6):
            self.c[k].wait_recv()

    def drain(self):
        for c in self.c:
            c.wait_send()


def reduce_scatter(place, part, out, land, send, recv):
    s, y, z = place
    up, down, far = (y + 1) % 4, (y + 3) % 4, (y + 2) % 4
    o = 1 - z

    def copy(k, yy, zz):
        return remote(out.at[k], land.at[k], send.at[k], recv.at[k], (s, yy * 2 + zz))

    c = (
        copy(0, up, z),
        copy(1, down, z),
        copy(2, down, z),
        copy(3, up, z),
        copy(4, up, z),
        copy(5, down, z),
        copy(6, y, o),
    )
    out[0] = part(far * 2).astype(BF16)
    c[0].start()
    out[1] = part(far * 2 + 1).astype(BF16)
    c[1].start()
    out[3] = part(up * 2 + 1).astype(BF16)
    c[3].start()
    out[2] = part(down * 2).astype(BF16)
    c[2].start()
    mine_up = part(up * 2)
    mine_down = part(down * 2 + 1)
    c[0].wait_recv()
    out[4] = (land[0].astype(F32) + mine_up).astype(BF16)
    c[4].start()
    c[1].wait_recv()
    out[5] = (land[1].astype(F32) + mine_down).astype(BF16)
    c[5].start()
    other = part(y * 2 + o)
    own = part(y * 2 + z)
    for k in (2, 3, 4, 5):
        c[k].wait_recv()
    out[6] = (other + land[2 + o].astype(F32) + land[4 + o].astype(F32)).astype(BF16)
    c[6].start()
    own = own + land[2 + z].astype(F32) + land[4 + z].astype(F32)
    c[6].wait_recv()
    own = own + land[6].astype(F32)
    return own, c


def kernel(
    tok, wq, wk, wv, m_in, m_out, fg, mo, st, plan, gain, aq, ak, av, ao, out_ref,
    kf, qf, rf, tf, cf, wo, vbuf, hid, slope, hq, mob, mot, kt,
    rs_out, rs_land, gates, gbuf, rbuf, wbuf, wland, kv, qs, nrm, m_s, l_s, acc,
    g_send, g_recv, r_send, r_recv, w_send, w_recv, gt_send, gt_recv, a_send, a_recv, b_send, b_recv, k_send, k_recv,
):
    s, h = lax.axis_index("seq"), lax.axis_index("head")
    y, z = h // 2, h % 2
    place = (s, y, z)
    par = s % 2

    barrier = pltpu.get_barrier_semaphore()

    def greet_head(d, carry):
        pl.semaphore_signal(barrier, inc=1, device_id=(s, (h + d) % NH), device_id_type=MESH)
        return carry

    def greet_seq(d, carry):
        pl.semaphore_signal(barrier, inc=1, device_id=((s + d) % NS, h), device_id_type=MESH)
        return carry

    lax.fori_loop(1, NH, greet_head, 0)
    lax.fori_loop(1, NS, greet_seq, 0)

    kf[:, col(h)] = dot(tok[...], wk[...]).astype(BF16)
    hot = lax.broadcasted_iota(jnp.int32, (16, W), 0) == plan[0]

    def row(table):
        return jnp.sum(jnp.where(hot, table[...], 0.0), axis=0, keepdims=True)

    gates[s] = jnp.concatenate([row(mo), 1.0 - row(fg), jnp.zeros((6, W), F32)], axis=0)
    rate = row(st)
    pl.semaphore_wait(barrier, NH - 1 + NS - 1)

    gk = Gather(place, kf, g_send.at[0], g_recv.at[0])
    gq = Gather(place, qf, g_send.at[1], g_recv.at[1])
    gr = Gather(place, rf, g_send.at[2], g_recv.at[2])
    gt = Gather(place, tf, g_send.at[3], g_recv.at[3])
    gc = Gather(place, cf, g_send.at[4], g_recv.at[4])
    gk.start()

    def send_gates(d, carry):
        remote(gates.at[s], gates.at[s], gt_send, gt_recv, ((s + d) % NS, h)).start()
        return carry

    lax.fori_loop(1, NS, send_gates, 0)
    qf[:, col(h)] = dot(tok[...], wq[...]).astype(BF16)
    vbuf[...] = dot(tok[...], wv[...]).astype(BF16)
    mob[...] = m_out[...].astype(BF16)
    gk.relay()
    mot[...] = m_out[...].T
    gk.finish()

    pre = dot(kf[...], m_in[...].astype(BF16))
    sig = jax.nn.sigmoid(pre)
    hid[...] = (pre * sig).astype(BF16)
    slope[...] = sig * (1.0 + pre * (1.0 - sig))

    def part_one(b):
        return dot(hid[...], mob[:, col(b)])

    predicted, sent_one = reduce_scatter(place, part_one, rs_out.at[0], rs_land.at[0], r_send.at[0], r_recv.at[0])
    rf[:, col(h)] = ((2.0 / T) * (predicted - vbuf[...].astype(F32))).astype(BF16)
    gr.start()
    kt[...] = kf[...].T
    gr.relay()
    gr.finish()

    g_out = dot(hid[...].T, rf[...])
    gbuf[:, 32:64, :] = (g_out.T * -rate).astype(BF16).reshape(NS, 32, W)
    term = (dot(rf[...], mob[...], NT) * slope[...]).astype(BF16)
    gbuf[:, 0:32, :] = (dot(kt[...], term) * -rate).astype(BF16).reshape(NS, 32, W)

    def send_grad(d, carry):
        o = (s + d) % NS
        remote(gbuf.at[o], rbuf.at[s], a_send, a_recv.at[s], (o, h)).start()
        return carry

    lax.fori_loop(1, NS, send_grad, 0)
    rbuf[s] = gbuf[s]
    gq.start()

    def wo_copy(d):
        p = (h + d) % NH
        return remote(ao.at[:, col(p)], wo.at[pl.ds(pl.multiple_of(h * W, W), W), :], w_send.at[d - 1], w_recv.at[d - 1], (s, p))

    for d in range(1, NH):
        wo_copy(d).start()
    wo[pl.ds(pl.multiple_of(h * W, W), W), :] = ao[:, col(h)]

    pltpu.make_async_copy(gates.at[pl.ds(0, NS - 1)], gates.at[pl.ds(0, NS - 1)], gt_recv).wait()

    rows = pl.ds(pl.multiple_of(s * 32, 32), 32)
    weight0 = jnp.concatenate([m_in[rows, :], mot[rows, :]], axis=0)

    def step(c, carry):
        speed, weight = carry
        wbuf[c] = weight.astype(BF16)

        @pl.when(c != s)
        def _():
            remote(wbuf.at[c], wland.at[s], b_send, b_recv, (c, h)).start()
            remote(gbuf.at[c], rbuf.at[c], a_send, a_recv.at[c], (c, h)).wait_recv()

        g = gates[c]
        speed = g[0:1] * speed + rbuf[c].astype(F32)
        weight = g[1:2] * weight + speed
        return speed, weight

    lax.fori_loop(0, NS, step, (jnp.zeros((64, W), F32), weight0))
    wland[s] = wbuf[s]
    gq.relay()
    gq.finish()
    some = pl.ds(0, NS - 1)
    pltpu.make_async_copy(wland.at[some], wland.at[some], b_recv).wait()

    act = dot(qf[...], wland[:, 0:32, :].reshape(1024, W))
    hq[...] = (act * jax.nn.sigmoid(act)).astype(BF16)

    def part_two(b):
        return dot(hq[...], wland[pl.ds(b * 4, 4), 32:64, :].reshape(W, W), NT)

    retrieved, sent_two = reduce_scatter(place, part_two, rs_out.at[1], rs_land.at[1], r_send.at[1], r_recv.at[1])
    tf[:, col(h)] = retrieved.astype(BF16)
    gt.start()
    gt.relay()
    gt.finish()
    for i in range(4):
        r = slice(i * 128, (i + 1) * 128)
        x = tf[r, :].astype(F32)
        mean = jnp.mean(x * x, axis=-1, keepdims=True)
        nrm[r, :] = (x * lax.rsqrt(mean + EPS) * gain[...]).astype(BF16)
    kv[0, :, 0:W] = dot(nrm[...], ak[...]).astype(BF16)
    kv[0, :, W : 2 * W] = dot(nrm[...], av[...]).astype(BF16)

    def own_copy(k):
        return remote(kv.at[0], kv.at[2 * k], k_send.at[k], k_recv.at[2 * k], (s + 2 * k, h))

    def side_copy():
        return remote(kv.at[0], kv.at[1], k_send.at[0], k_recv.at[1], (s + 1, h))

    def pass_copy(k):
        to = 2 * k + 1 - 2 * par
        return remote(kv.at[2 * k], kv.at[to], k_send.at[4 + k], k_recv.at[to], (s + 1 - 2 * par, h))

    def passes(k):
        return (s >= 2 * k) & ((par == 1) | (k < 4))

    for k in range(1, 5):

        @pl.when(s + 2 * k < NS)
        def _():
            own_copy(k).start()

    @pl.when(par == 0)
    def _():
        side_copy().start()

    query = dot(nrm[...], aq[...]).astype(BF16) * 0.125
    low = lax.broadcasted_iota(jnp.int32, (T, W), 1) < 64
    zero = jnp.zeros_like(query)
    qs[0] = jnp.where(low, query, zero)
    qs[1] = jnp.where(low, zero, query)
    m_s[...] = jnp.full_like(m_s, -1e30)
    l_s[...] = jnp.zeros_like(l_s)
    acc[...] = jnp.zeros_like(acc)

    def attend(slot, mode):
        for hd in range(2):
            for i in range(4):
                r = slice(i * 128, (i + 1) * 128)
                sc = dot(qs[hd, r, :], kv[slot, :, 0:W], NT)
                if mode != 1:
                    iq = lax.broadcasted_iota(jnp.int32, (128, T), 0) + i * 128
                    ik = lax.broadcasted_iota(jnp.int32, (128, T), 1)
                    sc = jnp.where(iq >= ik if mode == 0 else ik > iq, sc, -1e30)
                m_old = m_s[hd, r, :]
                m_new = jnp.maximum(m_old, jnp.max(sc, axis=-1, keepdims=True))
                p = jnp.exp(sc - m_new)
                fade = jnp.exp(m_old - m_new)
                m_s[hd, r, :] = m_new
                l_s[hd, r, :] = fade * l_s[hd, r, :] + jnp.sum(p, axis=-1, keepdims=True)
                acc[hd, r, :] = fade * acc[hd, r, :] + dot(p.astype(BF16), kv[slot, :, W : 2 * W])

    attend(0, 0)

    def arrive(slot):
        remote(kv.at[0], kv.at[slot], k_send.at[0], k_recv.at[slot], (s, h ^ 1)).wait_recv()

    def pair(k, mode):
        @pl.when(s >= 2 * k)
        def _():
            arrive(2 * k)

            @pl.when(passes(k))
            def _():
                pass_copy(k).start()

            attend(2 * k, mode)

        @pl.when(s >= 2 * k - 1)
        def _():
            arrive(2 * k - 1)
            attend(2 * k - 1, 1)

    def middle(k, carry):
        pair(k, 1)
        return carry

    lax.fori_loop(1, 4, middle, 0)
    pair(4, 2)
    cf[:, col(h)] = jnp.where(low, acc[0] / l_s[0], acc[1] / l_s[1]).astype(BF16)
    gc.start()
    gc.relay()
    for d in range(1, NH):
        wo_copy(d).wait_recv()
    gc.finish()
    out_ref[...] = dot(cf[...], wo[...]).astype(BF16)

    for g in (gk, gq, gr, gt, gc):
        g.drain()
    for c in sent_one + sent_two:
        c.wait_send()
    for d in range(1, NH):
        wo_copy(d).wait_send()
    pltpu.make_async_copy(gates.at[some], gates.at[some], gt_send).wait()
    pltpu.make_async_copy(gbuf.at[some], gbuf.at[some], a_send).wait()
    pltpu.make_async_copy(wbuf.at[some], wbuf.at[some], b_send).wait()
    for k in range(1, 5):

        @pl.when(s + 2 * k < NS)
        def _():
            own_copy(k).wait_send()

        @pl.when(passes(k))
        def _():
            pass_copy(k).wait_send()

    @pl.when(par == 0)
    def _():
        side_copy().wait_send()


def block(
    tokens, mem_query_w, mem_key_w, mem_value_w, mem_in, mem_out, forget_levels, momentum_levels, step_levels,
    plan, norm_gain, attn_query_w, attn_key_w, attn_value_w, attn_out_w,
):
    vm = pl.BlockSpec(memory_space=pltpu.VMEM)
    sm = pl.BlockSpec(memory_space=pltpu.SMEM)
    V = pltpu.VMEM
    dma = pltpu.SemaphoreType.DMA
    big = V((T, 1024), BF16)
    slab = V((NS, 64, W), BF16)
    return pl.pallas_call(
        kernel,
        name="titans",
        out_shape=jax.ShapeDtypeStruct((T, W), BF16),
        in_specs=[vm] * 9 + [sm] + [vm] * 5,
        out_specs=vm,
        scratch_shapes=[
            big, big, big, big, big,
            V((1024, W), BF16), V((T, W), BF16), V((T, W), BF16), V((T, W), F32), V((T, W), BF16),
            V((W, 1024), BF16), V((1024, W), F32), V((1024, T), BF16),
            V((2, 7, T, W), BF16), V((2, 7, T, W), BF16), V((NS, 8, W), F32),
            slab, slab, slab, slab,
            V((9, T, 2 * W), BF16), V((2, T, W), BF16), big, V((2, T, 1), F32), V((2, T, 1), F32), V((2, T, W), F32),
            dma((5, 7)), dma((5, 7)), dma((2, 7)), dma((2, 7)), dma((7,)), dma((7,)), dma, dma,
            dma, dma((NS,)), dma, dma, dma((9,)), dma((9,)),
        ],
        compiler_params=pltpu.CompilerParams(collective_id=0, has_side_effects=True, vmem_limit_bytes=60 * 1024 * 1024),
    )(
        tokens, mem_query_w, mem_key_w, mem_value_w, mem_in, mem_out, forget_levels, momentum_levels, step_levels,
        plan, norm_gain.reshape(1, -1), attn_query_w, attn_key_w, attn_value_w, attn_out_w,
    )


def solution(mesh):
    seq, head = P("seq", None), P(None, "head")
    in_specs = (
        seq, head, head, head, head, P("head", None), head, head, head, P("seq"), P(), head, head, head, P("head", None),
    )
    return jax.shard_map(block, mesh=mesh, in_specs=in_specs, out_specs=P("seq", "head"), check_vma=False)
```

```python
import jax
import jax.numpy as jnp
from jax import lax
from jax.experimental import pallas as pl
from jax.experimental.pallas import tpu as pltpu
from jax.sharding import PartitionSpec as P

MESH = pl.DeviceIdType.MESH
F32 = jnp.float32
BF16 = jnp.bfloat16
EPS = 1e-06
NS = 32
NH = 8
T = 512
W = 128
NN = (((1,), (0,)), ((), ()))
NT = (((1,), (1,)), ((), ()))


def dot(a, b, dims=NN):
    return lax.dot_general(a, b, dims, preferred_element_type=F32)


def col(b):
    return pl.ds(pl.multiple_of(b * W, W), W)


def remote(src, dst, send, recv, device):
    return pltpu.make_async_remote_copy(
        src_ref=src, dst_ref=dst, send_sem=send, recv_sem=recv, device_id=device, device_id_type=MESH
    )


class Gather:
    def __init__(self, place, buf, send, recv):
        s, y, z = place
        self.buf, self.send, self.recv = buf, send, recv
        self.up, self.down, self.far = (y + 1) % 4, (y + 3) % 4, (y + 2) % 4
        self.s, self.y, self.z = s, y, z

    def copy(self, block, sem, yy, zz):
        ref = self.buf.at[:, col(block)]
        return remote(ref, ref, self.send.at[sem], self.recv.at[sem], (self.s, yy * 2 + zz))

    def copies(self):
        s, y, z = self.s, self.y, self.z
        o = 1 - z
        return (
            self.copy(y * 2 + z, 0, y, o),
            self.copy(y * 2 + z, 1, self.up, z),
            self.copy(y * 2 + z, 2, self.down, z),
            self.copy(y * 2 + o, 3, self.up, z),
            self.copy(y * 2 + o, 4, self.down, z),
            self.copy(self.down * 2 + z, 5, self.up, z),
            self.copy(self.up * 2 + o, 6, self.down, z),
        )

    def start(self):
        self.c = self.copies()
        for k in (1, 2, 0):
            self.c[k].start()

    def relay_near(self):
        self.c[1].wait_recv()
        self.c[5].start()
        self.c[0].wait_recv()
        self.c[3].start()
        self.c[4].start()

    def relay_far(self):
        self.c[4].wait_recv()
        self.c[6].start()

    def relay(self):
        self.relay_near()
        self.relay_far()

    def finish(self):
        for k in (2, 3, 5, 6):
            self.c[k].wait_recv()

    def drain(self):
        for c in self.c:
            c.wait_send()


def reduce_scatter(place, part, out, land, send, recv):
    s, y, z = place
    up, down, far = (y + 1) % 4, (y + 3) % 4, (y + 2) % 4
    o = 1 - z

    def copy(k, yy, zz):
        return remote(out.at[k], land.at[k], send.at[k], recv.at[k], (s, yy * 2 + zz))

    c = (
        copy(0, up, z),
        copy(1, down, z),
        copy(2, down, z),
        copy(3, up, z),
        copy(4, up, z),
        copy(5, down, z),
        copy(6, y, o),
    )
    out[0] = part(far * 2).astype(BF16)
    c[0].start()
    out[1] = part(far * 2 + 1).astype(BF16)
    c[1].start()
    out[3] = part(up * 2 + 1).astype(BF16)
    c[3].start()
    out[2] = part(down * 2).astype(BF16)
    c[2].start()
    mine_up = part(up * 2)
    mine_down = part(down * 2 + 1)
    c[0].wait_recv()
    out[4] = (land[0].astype(F32) + mine_up).astype(BF16)
    c[4].start()
    c[1].wait_recv()
    out[5] = (land[1].astype(F32) + mine_down).astype(BF16)
    c[5].start()
    other = part(y * 2 + o)
    own = part(y * 2 + z)
    for k in (2, 3, 4, 5):
        c[k].wait_recv()
    out[6] = (other + land[2 + o].astype(F32) + land[4 + o].astype(F32)).astype(BF16)
    c[6].start()
    own = own + land[2 + z].astype(F32) + land[4 + z].astype(F32)
    c[6].wait_recv()
    own = own + land[6].astype(F32)
    return own, c


def kernel(
    tok, wq, wk, wv, m_in, m_out, fg, mo, st, plan, gain, aq, ak, av, ao, out_ref,
    kf, qf, rf, tf, cf, wo, vbuf, hid, slope, hq, mob, mot, kt,
    rs_out, rs_land, gates, gbuf, rbuf, wbuf, wland, kv, qs, nrm, m_s, acc,
    g_send, g_recv, r_send, r_recv, w_send, w_recv, gt_send, gt_recv, a_send, a_recv, b_send, b_recv, k_send, k_recv,
):
    s, h = lax.axis_index("seq"), lax.axis_index("head")
    y, z = h // 2, h % 2
    place = (s, y, z)
    par = s % 2

    barrier = pltpu.get_barrier_semaphore()

    def greet_head(d, carry):
        pl.semaphore_signal(barrier, inc=1, device_id=(s, (h + d) % NH), device_id_type=MESH)
        return carry

    def greet_seq(d, carry):
        pl.semaphore_signal(barrier, inc=1, device_id=((s + d) % NS, h), device_id_type=MESH)
        return carry

    lax.fori_loop(1, NH, greet_head, 0)
    lax.fori_loop(1, NS, greet_seq, 0)

    kf[:, col(h)] = dot(tok[...], wk[...]).astype(BF16)
    hot = lax.broadcasted_iota(jnp.int32, (16, W), 0) == plan[0]

    def row(table):
        return jnp.sum(jnp.where(hot, table[...], 0.0), axis=0, keepdims=True)

    gates[s] = jnp.concatenate([row(mo), 1.0 - row(fg), jnp.zeros((6, W), F32)], axis=0)
    rate = row(st)
    pl.semaphore_wait(barrier, NH - 1 + NS - 1)

    gk = Gather(place, kf, g_send.at[0], g_recv.at[0])
    gq = Gather(place, qf, g_send.at[1], g_recv.at[1])
    gr = Gather(place, rf, g_send.at[2], g_recv.at[2])
    gt = Gather(place, tf, g_send.at[3], g_recv.at[3])
    gc = Gather(place, cf, g_send.at[4], g_recv.at[4])
    gk.start()

    def send_gates(d, carry):
        remote(gates.at[s], gates.at[s], gt_send, gt_recv, ((s + d) % NS, h)).start()
        return carry

    lax.fori_loop(1, NS, send_gates, 0)
    qf[:, col(h)] = dot(tok[...], wq[...]).astype(BF16)
    vbuf[...] = dot(tok[...], wv[...]).astype(BF16)
    mob[...] = m_out[...].astype(BF16)
    gk.relay()
    mot[...] = m_out[...].T
    gk.finish()

    pre = dot(kf[...], m_in[...].astype(BF16))
    sig = jax.nn.sigmoid(pre)
    hid[...] = (pre * sig).astype(BF16)
    slope[...] = sig * (1.0 + pre * (1.0 - sig))

    def part_one(b):
        return dot(hid[...], mob[:, col(b)])

    predicted, sent_one = reduce_scatter(place, part_one, rs_out.at[0], rs_land.at[0], r_send.at[0], r_recv.at[0])
    rf[:, col(h)] = ((2.0 / T) * (predicted - vbuf[...].astype(F32))).astype(BF16)
    gr.start()
    kt[...] = kf[...].T
    gr.relay()
    gq.start()
    gr.finish()

    g_out = dot(hid[...].T, rf[...])
    gbuf[:, 32:64, :] = (g_out.T * -rate).astype(BF16).reshape(NS, 32, W)
    term = (dot(rf[...], mob[...], NT) * slope[...]).astype(BF16)
    gbuf[:, 0:32, :] = (dot(kt[...], term) * -rate).astype(BF16).reshape(NS, 32, W)

    def send_grad(d, carry):
        o = (s + d) % NS
        remote(gbuf.at[o], rbuf.at[s], a_send, a_recv.at[s], (o, h)).start()
        return carry

    lax.fori_loop(1, NS, send_grad, 0)
    rbuf[s] = gbuf[s]

    def wo_copy(d):
        p = (h + d) % NH
        return remote(ao.at[:, col(p)], wo.at[pl.ds(pl.multiple_of(h * W, W), W), :], w_send.at[d - 1], w_recv.at[d - 1], (s, p))

    for d in range(1, NH):
        wo_copy(d).start()
    wo[pl.ds(pl.multiple_of(h * W, W), W), :] = ao[:, col(h)]

    pltpu.make_async_copy(gates.at[pl.ds(0, NS - 1)], gates.at[pl.ds(0, NS - 1)], gt_recv).wait()

    rows = pl.ds(pl.multiple_of(s * 32, 32), 32)
    weight0 = jnp.concatenate([m_in[rows, :], mot[rows, :]], axis=0)

    def step(c, carry):
        speed, weight = carry
        wbuf[c] = weight.astype(BF16)

        @pl.when(c != s)
        def _():
            remote(wbuf.at[c], wland.at[s], b_send, b_recv, (c, h)).start()
            remote(gbuf.at[c], rbuf.at[c], a_send, a_recv.at[c], (c, h)).wait_recv()

        g = gates[c]
        speed = g[0:1] * speed + rbuf[c].astype(F32)
        weight = g[1:2] * weight + speed
        return speed, weight

    state = lax.fori_loop(0, 4, step, (jnp.zeros((64, W), F32), weight0))
    gq.relay_near()
    state = lax.fori_loop(4, 20, step, state)
    gq.relay_far()
    lax.fori_loop(20, NS, step, state)
    wland[s] = wbuf[s]
    gq.finish()
    some = pl.ds(0, NS - 1)
    pltpu.make_async_copy(wland.at[some], wland.at[some], b_recv).wait()

    act = dot(qf[...], wland[:, 0:32, :].reshape(1024, W))
    hq[...] = (act * jax.nn.sigmoid(act)).astype(BF16)

    def part_two(b):
        return dot(hq[...], wland[pl.ds(b * 4, 4), 32:64, :].reshape(W, W), NT)

    retrieved, sent_two = reduce_scatter(place, part_two, rs_out.at[1], rs_land.at[1], r_send.at[1], r_recv.at[1])
    tf[:, col(h)] = retrieved.astype(BF16)
    gt.start()
    gt.relay()
    gt.finish()
    for i in range(4):
        r = slice(i * 128, (i + 1) * 128)
        x = tf[r, :].astype(F32)
        mean = jnp.mean(x * x, axis=-1, keepdims=True)
        nrm[r, :] = (x * lax.rsqrt(mean + EPS) * gain[...]).astype(BF16)
    kv[0, :, 0:W] = dot(nrm[...], ak[...]).astype(BF16)
    kv[0, :, W : 2 * W] = dot(nrm[...], av[...]).astype(BF16)

    zl = (s // 2) % 4

    def own_copy(k):
        return remote(kv.at[0], kv.at[2 * k], k_send.at[k], k_recv.at[2 * k], (s + 2 * k, h))

    def side_copy():
        return remote(kv.at[0], kv.at[1], k_send.at[0], k_recv.at[1], (s + 1, h))

    def pass_copy(k):
        to = 2 * k + 1 - 2 * par
        return remote(kv.at[2 * k], kv.at[to], k_send.at[4 + k], k_recv.at[to], (s + 1 - 2 * par, h))

    def relay_copy(up):
        to = 6 if up else 2
        return remote(kv.at[4], kv.at[to], k_send.at[9], k_recv.at[to], (s + 2 if up else s - 2, h))

    def sends(k):
        ok = s + 2 * k < NS
        if k == 3:
            ok = ok & (zl != 0)
        if k == 1:
            ok = ok & (zl != 3)
        return ok

    def passes(k):
        return (s >= 2 * k) & ((par == 1) | (k < 4))

    for k in (2, 1, 3, 4):

        @pl.when(sends(k))
        def _():
            own_copy(k).start()

    @pl.when(par == 0)
    def _():
        side_copy().start()

    query = dot(nrm[...], aq[...]).astype(BF16) * 0.125
    low = lax.broadcasted_iota(jnp.int32, (128, W), 1) < 64
    for i in range(4):
        part = query[i * 128 : (i + 1) * 128, :]
        qs[i, 0:128, :] = jnp.where(low, part, jnp.zeros_like(part))
        qs[i, 128:256, :] = jnp.where(low, jnp.zeros_like(part), part)
    m_s[...] = jnp.full_like(m_s, -1e30)
    acc[...] = jnp.zeros_like(acc)
    ones = jnp.ones((T, W), BF16)

    def attend(slot, mode, edge=None):
        values = jnp.concatenate([kv[slot, :, W : 2 * W], ones], axis=1)
        for i in range(4):
            sc = dot(qs[i], kv[slot, :, 0:W], NT)
            if mode != 1:
                iq = lax.broadcasted_iota(jnp.int32, (256, T), 0) % 128 + i * 128
                ik = lax.broadcasted_iota(jnp.int32, (256, T), 1)
                sc = jnp.where(iq >= ik if mode == 0 else ik - iq > edge, sc, -1e30)
            m_old = m_s[i]
            m_new = jnp.maximum(m_old, jnp.max(sc, axis=-1, keepdims=True))
            p = jnp.exp(sc - m_new)
            m_s[i] = m_new
            acc[i] = jnp.exp(m_old - m_new) * acc[i] + dot(p.astype(BF16), values)

    attend(0, 0)
    def arrive(slot):
        remote(kv.at[0], kv.at[slot], k_send.at[0], k_recv.at[slot], (s, h ^ 1)).wait_recv()

    last = jnp.where(zl == 0, 1, 3)

    def chip(j):
        return jnp.where(j == 0, 2, jnp.where(j == 1, 4, jnp.where(j == 2, 4 - last, last)))

    def turn(j, carry):
        k = chip(j)
        odd = jnp.where(j == 0, par, 2 * chip(j - 1) - 1 + 2 * par)

        @pl.when((j < 4) & (s >= 2 * k))
        def _():
            arrive(2 * k)

            @pl.when((k == 2) & (zl == 2))
            def _():
                relay_copy(True).start()

            @pl.when((k == 2) & (zl == 1))
            def _():
                relay_copy(False).start()

            @pl.when(passes(k))
            def _():
                pass_copy(k).start()

            attend(2 * k, 2, jnp.where(k == 4, 0, -2 * T))

        @pl.when((odd > 0) & (odd < 9) & (s >= odd))
        def _():
            arrive(odd)
            attend(odd, 1)

        return carry

    lax.fori_loop(0, 5, turn, 0)
    for i in range(4):
        both = acc[i, :, 0:W] / acc[i, :, W : 2 * W]
        cf[i * 128 : (i + 1) * 128, col(h)] = jnp.where(low, both[0:128], both[128:256]).astype(BF16)
    gc.start()
    gc.relay()
    for d in range(1, NH):
        wo_copy(d).wait_recv()
    gc.finish()
    out_ref[...] = dot(cf[...], wo[...]).astype(BF16)

    for g in (gk, gq, gr, gt, gc):
        g.drain()
    for c in sent_one + sent_two:
        c.wait_send()
    for d in range(1, NH):
        wo_copy(d).wait_send()
    pltpu.make_async_copy(gates.at[some], gates.at[some], gt_send).wait()
    pltpu.make_async_copy(gbuf.at[some], gbuf.at[some], a_send).wait()
    pltpu.make_async_copy(wbuf.at[some], wbuf.at[some], b_send).wait()
    for k in range(1, 5):

        @pl.when(sends(k))
        def _():
            own_copy(k).wait_send()

        @pl.when(passes(k))
        def _():
            pass_copy(k).wait_send()

    @pl.when(par == 0)
    def _():
        side_copy().wait_send()

    @pl.when((s >= 4) & (zl == 2))
    def _():
        relay_copy(True).wait_send()

    @pl.when((s >= 4) & (zl == 1))
    def _():
        relay_copy(False).wait_send()


def block(
    tokens, mem_query_w, mem_key_w, mem_value_w, mem_in, mem_out, forget_levels, momentum_levels, step_levels,
    plan, norm_gain, attn_query_w, attn_key_w, attn_value_w, attn_out_w,
):
    vm = pl.BlockSpec(memory_space=pltpu.VMEM)
    sm = pl.BlockSpec(memory_space=pltpu.SMEM)
    V = pltpu.VMEM
    dma = pltpu.SemaphoreType.DMA
    big = V((T, 1024), BF16)
    slab = V((NS, 64, W), BF16)
    return pl.pallas_call(
        kernel,
        name="titans",
        out_shape=jax.ShapeDtypeStruct((T, W), BF16),
        in_specs=[vm] * 9 + [sm] + [vm] * 5,
        out_specs=vm,
        scratch_shapes=[
            big, big, big, big, big,
            V((1024, W), BF16), V((T, W), BF16), V((T, W), BF16), V((T, W), F32), V((T, W), BF16),
            V((W, 1024), BF16), V((1024, W), F32), V((1024, T), BF16),
            V((2, 7, T, W), BF16), V((2, 7, T, W), BF16), V((NS, 8, W), F32),
            slab, slab, slab, slab,
            V((9, T, 2 * W), BF16), V((4, 256, W), BF16), big, V((4, 256, 1), F32), V((4, 256, 2 * W), F32),
            dma((5, 7)), dma((5, 7)), dma((2, 7)), dma((2, 7)), dma((7,)), dma((7,)), dma, dma,
            dma, dma((NS,)), dma, dma, dma((10,)), dma((9,)),
        ],
        compiler_params=pltpu.CompilerParams(collective_id=0, has_side_effects=True, vmem_limit_bytes=60 * 1024 * 1024),
    )(
        tokens, mem_query_w, mem_key_w, mem_value_w, mem_in, mem_out, forget_levels, momentum_levels, step_levels,
        plan, norm_gain.reshape(1, -1), attn_query_w, attn_key_w, attn_value_w, attn_out_w,
    )


def solution(mesh):
    seq, head = P("seq", None), P(None, "head")
    in_specs = (
        seq, head, head, head, head, P("head", None), head, head, head, P("seq"), P(), head, head, head, P("head", None),
    )
    return jax.shard_map(block, mesh=mesh, in_specs=in_specs, out_specs=P("seq", "head"), check_vma=False)
```

```python
import jax
import jax.numpy as jnp
from jax import lax
from jax.experimental import pallas as pl
from jax.experimental.pallas import tpu as pltpu
from jax.sharding import PartitionSpec as P

MESH = pl.DeviceIdType.MESH
F32 = jnp.float32
BF16 = jnp.bfloat16
EPS = 1e-06
NS = 32
NH = 8
T = 512
W = 128
NN = (((1,), (0,)), ((), ()))
NT = (((1,), (1,)), ((), ()))


def dot(a, b, dims=NN):
    return lax.dot_general(a, b, dims, preferred_element_type=F32)


def col(b):
    return pl.ds(pl.multiple_of(b * W, W), W)


def remote(src, dst, send, recv, device):
    return pltpu.make_async_remote_copy(
        src_ref=src, dst_ref=dst, send_sem=send, recv_sem=recv, device_id=device, device_id_type=MESH
    )


HALF = T // 2
PARTS = 2


def half(c):
    return pl.ds(c * HALF, HALF)


class Ring:
    def __init__(self, place, bit, buf, send, recv):
        self.s, self.y, self.z = place
        self.a, self.b = bit, 1 - bit
        self.buf, self.send, self.recv = buf, send, recv

    def copy(self, c, k):
        y, a, b = self.y, self.a, self.b
        up, down = (y + 1) % 4, (y + 3) % 4
        block, to = ((y * 2 + a, up), (y * 2 + a, down), (y * 2 + b, up), (y * 2 + b, down), (down * 2 + a, up), (up * 2 + b, down))[k]
        ref = self.buf.at[half(c), col(block)]
        return remote(ref, ref, self.send.at[c, k], self.recv.at[c, k], (self.s, to * 2 + self.z))

    def give_a(self, c):
        self.copy(c, 0).start()
        self.copy(c, 1).start()

    def give_b(self, c):
        self.copy(c, 2).start()
        self.copy(c, 3).start()

    def relay(self, c):
        self.copy(c, 0).wait_recv()
        self.copy(c, 4).start()
        self.copy(c, 3).wait_recv()
        self.copy(c, 5).start()

    def finish(self, c):
        for k in (1, 2, 4, 5):
            self.copy(c, k).wait_recv()

    def drain(self):
        for c in range(PARTS):
            for k in range(6):
                self.copy(c, k).wait_send()


class Core:
    def __init__(self, place):
        self.s, self.y, self.z = place
        self.k = self.s % 2
        up, down = (self.y + 1) % 4, (self.y + 3) % 4
        self.far = (self.y + 2) % 4
        self.next = jnp.where(self.k == 0, up, down)
        self.prev = jnp.where(self.k == 0, down, up)

    def at(self, y):
        return (self.s, y * 2 + self.z)

    def other(self):
        return (self.s + 1 - 2 * self.k, self.y * 2 + self.z)


def gather(core, buf, send, recv):
    me, k = core, core.k

    def copy(n, y, to):
        ref = buf.at[:, col(y * 2 + k)]
        return remote(ref, ref, send.at[n], recv.at[n], to)

    c = (
        copy(0, me.y, me.at(me.next)),
        copy(1, me.y, me.at(me.prev)),
        copy(2, me.prev, me.at(me.next)),
        copy(3, me.y, me.other()),
        copy(4, me.prev, me.other()),
        copy(5, me.next, me.other()),
        copy(6, me.far, me.other()),
    )

    def start():
        for n in (0, 1, 3):
            c[n].start()

    def finish():
        c[0].wait_recv()
        c[2].start()
        c[4].start()
        c[1].wait_recv()
        c[5].start()
        c[2].wait_recv()
        c[6].start()
        for n in (3, 4, 5, 6):
            c[n].wait_recv()

    return start, finish, c


def reduce_scatter(core, part, out, land, send, recv):
    me, k = core, core.k

    def copy(n, to):
        return remote(out.at[n], land.at[n], send.at[n], recv.at[n], to)

    order = (me.far, me.next, me.prev, me.y)
    c = tuple(copy(n, me.other()) for n in range(4)) + (copy(4, me.at(me.next)), copy(5, me.at(me.next)), copy(6, me.at(me.prev)))
    slot = (0, 2, 1, 3)
    for n, y in enumerate(order):
        out[n] = part(y * 2 + 1 - k).astype(BF16)
        c[n].start()

    def chip(n):
        mine = part(order[n] * 2 + k)
        c[slot[n]].wait_recv()
        return mine + land[slot[n]].astype(F32)

    out[4] = chip(0).astype(BF16)
    c[4].start()
    out[6] = chip(2).astype(BF16)
    c[6].start()
    onward = chip(1)
    own = chip(3)
    c[4].wait_recv()
    out[5] = (land[4].astype(F32) + onward).astype(BF16)
    c[5].start()
    c[6].wait_recv()
    own = own + land[6].astype(F32)
    c[5].wait_recv()
    return own + land[5].astype(F32), c


def kernel(
    tok, wq, wk, wv, m_in, m_out, fg, mo, st, plan, gain, aq, ak, av, ao, out_ref,
    kf, qf, rf, tf, cf, wo, kb, qb, vb, tb, vbuf, hid, slope, hq, mi, mob, mot, w0, w0s, kt,
    rs_out, rs_land, gates, gown, gbuf, rbuf, wbuf, wland, kv, qs, nrm, m_s, acc,
    g_send, g_recv, h_send, h_recv, r_send, r_recv, p_send, p_recv, w_send, w_recv, gt_send, gt_recv,
    a_send, a_recv, b_send, b_recv, k_send, k_recv,
):
    s, h = lax.axis_index("seq"), lax.axis_index("head")
    y, z = h // 2, h % 2
    place = (s, y, z)
    par = s % 2
    home = par == z
    away = par != z
    g = s - par + z
    core = Core(place)
    across = (s, y * 2 + 1 - z)
    aside = core.other()
    pair = (s + 1 - 2 * par, y * 2 + 1 - z)

    def group(c):
        return (c // 2 * 2 + par, y * 2 + c % 2)

    def send(n, src, dst, to):
        return remote(src, dst, p_send.at[n], p_recv.at[n], to)

    barrier = pltpu.get_barrier_semaphore()

    def greet_head(d, carry):
        pl.semaphore_signal(barrier, inc=1, device_id=(s, (h + d) % NH), device_id_type=MESH)
        return carry

    def greet_seq(d, carry):
        pl.semaphore_signal(barrier, inc=1, device_id=group((g + d) % NS), device_id_type=MESH)
        return carry

    lax.fori_loop(1, NH, greet_head, 0)
    lax.fori_loop(1, NS, greet_seq, 0)
    for to in (aside, pair):
        pl.semaphore_signal(barrier, inc=1, device_id=to, device_id_type=MESH)

    key = dot(tok[...], wk[...]).astype(BF16)
    kb[...] = key

    @pl.when(home)
    def _():
        kf[:, col(h)] = key

    hot = lax.broadcasted_iota(jnp.int32, (16, W), 0) == plan[0]

    def row(table):
        return jnp.sum(jnp.where(hot, table[...], 0.0), axis=0, keepdims=True)

    gown[...] = jnp.concatenate([row(mo), 1.0 - row(fg), row(st), jnp.zeros((5, W), F32)], axis=0)
    pl.semaphore_wait(barrier, NH - 1 + NS - 1 + 2)

    ring_k = Ring(place, z, kf, g_send.at[0], g_recv.at[0])
    ring_q = Ring(place, z, qf, g_send.at[1], g_recv.at[1])
    ring_t = Ring(place, par, tf, g_send.at[2], g_recv.at[2])
    ring_c = Ring(place, z, cf, g_send.at[3], g_recv.at[3])

    def z_copy(n, c, src, dst):
        return send(n + c, src.at[half(c)], dst.at[half(c), col(h)], across)

    def side_rows(n, c, buf):
        return send(n + c, buf.at[half(c)], buf.at[half(c)], aside)

    def v_copy():
        return send(4, vb, vbuf, pair)

    def gate_copy():
        return send(5, gown, gates.at[s], pair)

    def mi_copy():
        return send(6, mi, mi, across)

    def mo_copy():
        return send(7, mob, mob, across)

    def w0_copy():
        return send(8, w0s, w0, across)

    @pl.when(home)
    def _():
        for c in range(PARTS):
            ring_k.give_a(c)
        mi[...] = m_in[...].astype(BF16)
        mob[...] = m_out[...].astype(BF16)

    @pl.when(away)
    def _():
        for c in range(PARTS):
            z_copy(0, c, kb, kf).start()

    query = dot(tok[...], wq[...]).astype(BF16)
    qb[...] = query
    value = dot(tok[...], wv[...]).astype(BF16)

    @pl.when(home)
    def _():
        mi_copy().start()
        mo_copy().start()
        mot[...] = m_out[...].T
        qf[:, col(h)] = query
        vbuf[...] = value
        gates[g] = gown[...]

        def rows(c):
            r = pl.ds(pl.multiple_of(c * 32, 32), 32)
            return jnp.concatenate([m_in[r, :], mot[r, :]], axis=0)

        w0[...] = rows(g)
        w0s[...] = rows(g + 1 - 2 * z)
        w0_copy().start()

    @pl.when(away)
    def _():
        vb[...] = value
        v_copy().start()
        gate_copy().start()

    @pl.when(home)
    def _():
        for c in range(PARTS):
            z_copy(0, c, kb, kf).wait_recv()
            ring_k.give_b(c)
        for c in range(PARTS):
            ring_k.relay(c)
        for c in range(PARTS):
            ring_k.finish(c)
            side_rows(9, c, kf).start()

    @pl.when(away)
    def _():
        mi_copy().wait_recv()
        mo_copy().wait_recv()
        for c in range(PARTS):
            side_rows(9, c, kf).wait_recv()
        for c in range(PARTS):
            z_copy(2, c, qb, qf).start()

    pre = dot(kf[...], mi[...])
    sig = jax.nn.sigmoid(pre)
    hid[...] = (pre * sig).astype(BF16)
    slope[...] = sig * (1.0 + pre * (1.0 - sig))

    def part_one(b):
        return dot(hid[...], mob[:, col(b)])

    predicted, sent_one = reduce_scatter(core, part_one, rs_out.at[0], rs_land.at[0], r_send.at[0], r_recv.at[0])

    @pl.when(away)
    def _():
        v_copy().wait_recv()
        gate_copy().wait_recv()
        w0_copy().wait_recv()

    own = core.y * 2 + par
    rf[:, col(own)] = ((2.0 / T) * (predicted - vbuf[...].astype(F32))).astype(BF16)
    r_start, r_finish, sent_r = gather(core, rf, h_send, h_recv)
    r_start()

    def send_gates(d, carry):
        remote(gates.at[g], gates.at[g], gt_send, gt_recv, group((g + d) % NS)).start()
        return carry

    lax.fori_loop(1, NS, send_gates, 0)
    kt[...] = kf[...].T
    r_finish()

    @pl.when(home)
    def _():
        for c in range(PARTS):
            ring_q.give_a(c)

    rate = gates[g][2:3]
    g_out = dot(hid[...].T, rf[...])
    gbuf[:, 32:64, :] = (g_out.T * -rate).astype(BF16).reshape(NS, 32, W)
    term = (dot(rf[...], mob[...], NT) * slope[...]).astype(BF16)
    gbuf[:, 0:32, :] = (dot(kt[...], term) * -rate).astype(BF16).reshape(NS, 32, W)

    def send_grad(d, carry):
        o = (g + d) % NS
        remote(gbuf.at[o], rbuf.at[g], a_send, a_recv.at[g], group(o)).start()
        return carry

    lax.fori_loop(1, NS, send_grad, 0)
    rbuf[g] = gbuf[g]

    def wo_copy(d):
        p = (h + d) % NH
        return remote(ao.at[:, col(p)], wo.at[pl.ds(pl.multiple_of(h * W, W), W), :], w_send.at[d - 1], w_recv.at[d - 1], (s, p))

    for d in range(1, NH):
        wo_copy(d).start()
    wo[pl.ds(pl.multiple_of(h * W, W), W), :] = ao[:, col(h)]

    pltpu.make_async_copy(gates.at[pl.ds(0, NS - 1)], gates.at[pl.ds(0, NS - 1)], gt_recv).wait()

    def step(c, carry):
        speed, weight = carry
        wbuf[c] = weight.astype(BF16)

        @pl.when(c != g)
        def _():
            remote(wbuf.at[c], wland.at[g], b_send, b_recv, group(c)).start()
            remote(gbuf.at[c], rbuf.at[c], a_send, a_recv.at[c], group(c)).wait_recv()

        gate = gates[c]
        speed = gate[0:1] * speed + rbuf[c].astype(F32)
        weight = gate[1:2] * weight + speed
        return speed, weight

    state = lax.fori_loop(0, 4, step, (jnp.zeros((64, W), F32), w0[...]))

    @pl.when(home)
    def _():
        for c in range(PARTS):
            z_copy(2, c, qb, qf).wait_recv()
            ring_q.give_b(c)

    state = lax.fori_loop(4, 20, step, state)

    @pl.when(home)
    def _():
        for c in range(PARTS):
            ring_q.relay(c)

    lax.fori_loop(20, NS, step, state)
    wland[g] = wbuf[g]
    @pl.when(home)
    def _():
        for c in range(PARTS):
            ring_q.finish(c)
            side_rows(11, c, qf).start()

    @pl.when(away)
    def _():
        for c in range(PARTS):
            side_rows(11, c, qf).wait_recv()

    some = pl.ds(0, NS - 1)
    pltpu.make_async_copy(wland.at[some], wland.at[some], b_recv).wait()

    act = dot(qf[...], wland[:, 0:32, :].reshape(1024, W))
    hq[...] = (act * jax.nn.sigmoid(act)).astype(BF16)

    def part_two(b):
        return dot(hq[...], wland[pl.ds(b * 4, 4), 32:64, :].reshape(W, W), NT)

    retrieved, sent_two = reduce_scatter(core, part_two, rs_out.at[1], rs_land.at[1], r_send.at[1], r_recv.at[1])

    tb[...] = retrieved.astype(BF16)

    def t_copy(n, c, to):
        return send(n + c, tb.at[half(c)], tf.at[half(c), col(own)], to)

    @pl.when(home)
    def _():
        for c in range(PARTS):
            t_copy(13, c, across).start()
        tf[:, col(own)] = tb[...]
        for c in range(PARTS):
            ring_t.give_a(c)
        for c in range(PARTS):
            t_copy(17, c, aside).wait_recv()
            ring_t.give_b(c)

    @pl.when(away)
    def _():
        for c in range(PARTS):
            t_copy(17, c, aside).start()
            t_copy(15, c, pair).start()
        for c in range(PARTS):
            t_copy(13, c, across).wait_recv()
            ring_t.give_a(c)
            t_copy(15, c, pair).wait_recv()
            ring_t.give_b(c)

    for c in range(PARTS):
        ring_t.relay(c)
    for c in range(PARTS):
        ring_t.finish(c)
    for i in range(4):
        r = slice(i * 128, (i + 1) * 128)
        x = tf[r, :].astype(F32)
        mean = jnp.mean(x * x, axis=-1, keepdims=True)
        nrm[r, :] = (x * lax.rsqrt(mean + EPS) * gain[...]).astype(BF16)
    kv[0, :, 0:W] = dot(nrm[...], ak[...]).astype(BF16)
    kv[0, :, W : 2 * W] = dot(nrm[...], av[...]).astype(BF16)

    zl = (s // 2) % 4

    def own_copy(k):
        return remote(kv.at[0], kv.at[2 * k], k_send.at[k], k_recv.at[2 * k], (s + 2 * k, h))

    def side_copy():
        return remote(kv.at[0], kv.at[1], k_send.at[0], k_recv.at[1], (s + 1, h))

    def pass_copy(k):
        to = 2 * k + 1 - 2 * par
        return remote(kv.at[2 * k], kv.at[to], k_send.at[4 + k], k_recv.at[to], (s + 1 - 2 * par, h))

    def relay_copy(up):
        to = 6 if up else 2
        return remote(kv.at[4], kv.at[to], k_send.at[9], k_recv.at[to], (s + 2 if up else s - 2, h))

    def sends(k):
        ok = s + 2 * k < NS
        if k == 3:
            ok = ok & (zl != 0)
        if k == 1:
            ok = ok & (zl != 3)
        return ok

    def passes(k):
        return (s >= 2 * k) & ((par == 1) | (k < 4))

    for k in (2, 1, 3, 4):

        @pl.when(sends(k))
        def _():
            own_copy(k).start()

    @pl.when(par == 0)
    def _():
        side_copy().start()

    query = dot(nrm[...], aq[...]).astype(BF16) * 0.125
    low = lax.broadcasted_iota(jnp.int32, (128, W), 1) < 64
    for i in range(4):
        part = query[i * 128 : (i + 1) * 128, :]
        qs[i, 0:128, :] = jnp.where(low, part, jnp.zeros_like(part))
        qs[i, 128:256, :] = jnp.where(low, jnp.zeros_like(part), part)
    m_s[...] = jnp.full_like(m_s, -1e30)
    acc[...] = jnp.zeros_like(acc)
    ones = jnp.ones((T, W), BF16)

    def attend(slot, mode, edge=None):
        values = jnp.concatenate([kv[slot, :, W : 2 * W], ones], axis=1)
        for i in range(4):
            sc = dot(qs[i], kv[slot, :, 0:W], NT)
            if mode != 1:
                iq = lax.broadcasted_iota(jnp.int32, (256, T), 0) % 128 + i * 128
                ik = lax.broadcasted_iota(jnp.int32, (256, T), 1)
                sc = jnp.where(iq >= ik if mode == 0 else ik - iq > edge, sc, -1e30)
            m_old = m_s[i]
            m_new = jnp.maximum(m_old, jnp.max(sc, axis=-1, keepdims=True))
            p = jnp.exp(sc - m_new)
            m_s[i] = m_new
            acc[i] = jnp.exp(m_old - m_new) * acc[i] + dot(p.astype(BF16), values)

    attend(0, 0)
    def arrive(slot):
        remote(kv.at[0], kv.at[slot], k_send.at[0], k_recv.at[slot], (s, h ^ 1)).wait_recv()

    last = jnp.where(zl == 0, 1, 3)

    def chip(j):
        return jnp.where(j == 0, 2, jnp.where(j == 1, 4, jnp.where(j == 2, 4 - last, last)))

    def turn(j, carry):
        k = chip(j)
        odd = jnp.where(j == 0, par, 2 * chip(j - 1) - 1 + 2 * par)

        @pl.when((j < 4) & (s >= 2 * k))
        def _():
            arrive(2 * k)

            @pl.when((k == 2) & (zl == 2))
            def _():
                relay_copy(True).start()

            @pl.when((k == 2) & (zl == 1))
            def _():
                relay_copy(False).start()

            @pl.when(passes(k))
            def _():
                pass_copy(k).start()

            attend(2 * k, 2, jnp.where(k == 4, 0, -2 * T))

        @pl.when((odd > 0) & (odd < 9) & (s >= odd))
        def _():
            arrive(odd)
            attend(odd, 1)

        return carry

    lax.fori_loop(0, 5, turn, 0)
    for i in range(4):
        both = acc[i, :, 0:W] / acc[i, :, W : 2 * W]
        cf[i * 128 : (i + 1) * 128, col(h)] = jnp.where(low, both[0:128], both[128:256]).astype(BF16)

    def c_copy(c):
        ref = cf.at[half(c), col(h)]
        return send(19 + c, ref, ref, across)

    for c in range(PARTS):
        c_copy(c).start()
        ring_c.give_a(c)
    for c in range(PARTS):
        c_copy(c).wait_recv()
        ring_c.give_b(c)
    for d in range(1, NH):
        wo_copy(d).wait_recv()
    for c in range(PARTS):
        ring_c.relay(c)
    for c in range(PARTS):
        ring_c.finish(c)
        out_ref[half(c), :] = dot(cf[half(c), :], wo[...]).astype(BF16)

    @pl.when(home)
    def _():
        ring_k.drain()
        ring_q.drain()
        for c in range(PARTS):
            side_rows(9, c, kf).wait_send()
            side_rows(11, c, qf).wait_send()
            t_copy(13, c, across).wait_send()
        mi_copy().wait_send()
        mo_copy().wait_send()
        w0_copy().wait_send()

    @pl.when(away)
    def _():
        for c in range(PARTS):
            z_copy(0, c, kb, kf).wait_send()
            z_copy(2, c, qb, qf).wait_send()
            t_copy(17, c, aside).wait_send()
            t_copy(15, c, pair).wait_send()
        v_copy().wait_send()
        gate_copy().wait_send()

    ring_t.drain()
    ring_c.drain()
    for c in range(PARTS):
        c_copy(c).wait_send()
    for c in sent_one + sent_two + sent_r:
        c.wait_send()
    for d in range(1, NH):
        wo_copy(d).wait_send()
    pltpu.make_async_copy(gates.at[some], gates.at[some], gt_send).wait()
    pltpu.make_async_copy(gbuf.at[some], gbuf.at[some], a_send).wait()
    pltpu.make_async_copy(wbuf.at[some], wbuf.at[some], b_send).wait()
    for k in range(1, 5):

        @pl.when(sends(k))
        def _():
            own_copy(k).wait_send()

        @pl.when(passes(k))
        def _():
            pass_copy(k).wait_send()

    @pl.when(par == 0)
    def _():
        side_copy().wait_send()

    @pl.when((s >= 4) & (zl == 2))
    def _():
        relay_copy(True).wait_send()

    @pl.when((s >= 4) & (zl == 1))
    def _():
        relay_copy(False).wait_send()


def block(
    tokens, mem_query_w, mem_key_w, mem_value_w, mem_in, mem_out, forget_levels, momentum_levels, step_levels,
    plan, norm_gain, attn_query_w, attn_key_w, attn_value_w, attn_out_w,
):
    vm = pl.BlockSpec(memory_space=pltpu.VMEM)
    sm = pl.BlockSpec(memory_space=pltpu.SMEM)
    V = pltpu.VMEM
    dma = pltpu.SemaphoreType.DMA
    big = V((T, 1024), BF16)
    slab = V((NS, 64, W), BF16)
    return pl.pallas_call(
        kernel,
        name="titans",
        out_shape=jax.ShapeDtypeStruct((T, W), BF16),
        in_specs=[vm] * 9 + [sm] + [vm] * 5,
        out_specs=vm,
        scratch_shapes=[
            big, big, big, big, big,
            V((1024, W), BF16), V((T, W), BF16), V((T, W), BF16), V((T, W), BF16), V((T, W), BF16), V((T, W), BF16),
            V((T, W), BF16), V((T, W), F32), V((T, W), BF16), V((1024, W), BF16), V((W, 1024), BF16), V((1024, W), F32),
            V((64, W), F32), V((64, W), F32), V((1024, T), BF16),
            V((2, 7, T, W), BF16), V((2, 7, T, W), BF16), V((NS, 8, W), F32), V((8, W), F32),
            slab, slab, slab, slab,
            V((9, T, 2 * W), BF16), V((4, 256, W), BF16), big, V((4, 256, 1), F32), V((4, 256, 2 * W), F32),
            dma((4, PARTS, 6)), dma((4, PARTS, 6)), dma((7,)), dma((7,)), dma((2, 7)), dma((2, 7)), dma((21,)), dma((21,)),
            dma((7,)), dma((7,)), dma, dma,
            dma, dma((NS,)), dma, dma, dma((10,)), dma((9,)),
        ],
        compiler_params=pltpu.CompilerParams(collective_id=0, has_side_effects=True, vmem_limit_bytes=60 * 1024 * 1024),
    )(
        tokens, mem_query_w, mem_key_w, mem_value_w, mem_in, mem_out, forget_levels, momentum_levels, step_levels,
        plan, norm_gain.reshape(1, -1), attn_query_w, attn_key_w, attn_value_w, attn_out_w,
    )


def solution(mesh):
    seq, head = P("seq", None), P(None, "head")
    in_specs = (
        seq, head, head, head, head, P("head", None), head, head, head, P("seq"), P(), head, head, head, P("head", None),
    )
    return jax.shard_map(block, mesh=mesh, in_specs=in_specs, out_specs=P("seq", "head"), check_vma=False)
```

```python
import jax
import jax.numpy as jnp
from jax import lax
from jax.experimental import pallas as pl
from jax.experimental.pallas import tpu as pltpu
from jax.sharding import PartitionSpec as P

MESH = pl.DeviceIdType.MESH
F32 = jnp.float32
BF16 = jnp.bfloat16
EPS = 1e-06
NS = 32
NH = 8
T = 512
W = 128
NN = (((1,), (0,)), ((), ()))
NT = (((1,), (1,)), ((), ()))


def dot(a, b, dims=NN):
    return lax.dot_general(a, b, dims, preferred_element_type=F32)


def col(b):
    return pl.ds(pl.multiple_of(b * W, W), W)


def remote(src, dst, send, recv, device):
    return pltpu.make_async_remote_copy(
        src_ref=src, dst_ref=dst, send_sem=send, recv_sem=recv, device_id=device, device_id_type=MESH
    )


HALF = T // 2
PARTS = 2


def half(c):
    return pl.ds(c * HALF, HALF)


class Ring:
    def __init__(self, place, bit, buf, send, recv):
        self.s, self.y, self.z = place
        self.a, self.b = bit, 1 - bit
        self.buf, self.send, self.recv = buf, send, recv

    def copy(self, c, k):
        y, a, b = self.y, self.a, self.b
        up, down = (y + 1) % 4, (y + 3) % 4
        block, to = ((y * 2 + a, up), (y * 2 + a, down), (y * 2 + b, up), (y * 2 + b, down), (down * 2 + a, up), (up * 2 + b, down))[k]
        ref = self.buf.at[half(c), col(block)]
        return remote(ref, ref, self.send.at[c, k], self.recv.at[c, k], (self.s, to * 2 + self.z))

    def give_a(self, c):
        self.copy(c, 0).start()
        self.copy(c, 1).start()

    def give_b(self, c):
        self.copy(c, 2).start()
        self.copy(c, 3).start()

    def relay(self, c):
        self.copy(c, 0).wait_recv()
        self.copy(c, 4).start()
        self.copy(c, 3).wait_recv()
        self.copy(c, 5).start()

    def finish(self, c):
        for k in (1, 2, 4, 5):
            self.copy(c, k).wait_recv()

    def drain(self):
        for c in range(PARTS):
            for k in range(6):
                self.copy(c, k).wait_send()


class Core:
    def __init__(self, place):
        self.s, self.y, self.z = place
        self.k = self.s % 2
        up, down = (self.y + 1) % 4, (self.y + 3) % 4
        self.far = (self.y + 2) % 4
        self.next = jnp.where(self.k == 0, up, down)
        self.prev = jnp.where(self.k == 0, down, up)

    def at(self, y):
        return (self.s, y * 2 + self.z)

    def other(self):
        return (self.s + 1 - 2 * self.k, self.y * 2 + self.z)


class Share:
    def __init__(self, core, buf, send, recv):
        self.me, self.buf, self.send, self.recv = core, buf, send, recv

    def copy(self, c, n):
        me = self.me
        y = (me.y, me.y, me.prev, me.y, me.prev, me.next, me.far)[n]
        to = (me.at(me.next), me.at(me.prev), me.at(me.next), me.other(), me.other(), me.other(), me.other())[n]
        ref = self.buf.at[half(c), col(y * 2 + me.k)]
        return remote(ref, ref, self.send.at[c, n], self.recv.at[c, n], to)

    def start(self, c):
        for n in (0, 1, 3):
            self.copy(c, n).start()

    def step(self, c):
        self.copy(c, 0).wait_recv()
        self.copy(c, 2).start()
        self.copy(c, 4).start()
        self.copy(c, 1).wait_recv()
        self.copy(c, 5).start()

    def last(self, c):
        self.copy(c, 2).wait_recv()
        self.copy(c, 6).start()

    def finish(self, c):
        for n in (3, 4, 5, 6):
            self.copy(c, n).wait_recv()

    def drain(self):
        for c in range(PARTS):
            for n in range(7):
                self.copy(c, n).wait_send()


class Sum:
    def __init__(self, core, part, out, land, send, recv):
        self.me, self.part, self.out, self.land, self.send, self.recv = core, part, out, land, send, recv
        self.order = (core.far, core.next, core.prev, core.y)

    def copy(self, c, n):
        me = self.me
        to = me.other() if n < 4 else me.at(me.prev if n == 6 else me.next)
        return remote(self.out.at[n, half(c)], self.land.at[n, half(c)], self.send.at[c, n], self.recv.at[c, n], to)

    def put(self, c, n, value):
        self.out[n, half(c), :] = value.astype(BF16)
        self.copy(c, n).start()

    def got(self, c, n):
        self.copy(c, n).wait_recv()
        return self.land[n, half(c), :].astype(F32)

    def give(self, c):
        for n, y in enumerate(self.order):
            self.put(c, n, self.part(c, y * 2 + 1 - self.me.k))

    def chip(self, c, n):
        return self.part(c, self.order[n] * 2 + self.me.k) + self.got(c, (0, 2, 1, 3)[n])

    def first(self, c):
        self.put(c, 4, self.chip(c, 0))
        self.put(c, 6, self.chip(c, 2))

    def second(self, c):
        onward = self.chip(c, 1)
        self.put(c, 5, self.got(c, 4) + onward)

    def last(self, c):
        own = self.chip(c, 3)
        return own + self.got(c, 6) + self.got(c, 5)

    def run(self):
        for stage in (self.give, self.first, self.second):
            for c in range(PARTS):
                stage(c)

    def drain(self):
        for c in range(PARTS):
            for n in range(7):
                self.copy(c, n).wait_send()


def kernel(
    tok_h, wq_h, wk_h, wv_h, m_in_h, m_out_h, fg, mo, st, plan, gain, aq_h, ak_h, av_h, ao_h, out_ref,
    tok, wk, wq, wv, m_in, m_out, aq, ak, av, ao, l_sem,
    kf, qf, rf, tf, cf, wo, kb, qb, vb, tb, vbuf, hid, slope, hq, mi, mob, mot, w0, w0s, kt,
    rs_out, rs_land, gates, gown, gbuf, rbuf, wbuf, wland, kv, qs, nrm, m_s, acc,
    g_send, g_recv, h_send, h_recv, r_send, r_recv, p_send, p_recv, w_send, w_recv, gt_send, gt_recv,
    a_send, a_recv, b_send, b_recv, k_send, k_recv, x_send, x_recv,
):
    s, h = lax.axis_index("seq"), lax.axis_index("head")
    y, z = h // 2, h % 2
    place = (s, y, z)
    par = s % 2
    home = par == z
    away = par != z
    g = s - par + z
    core = Core(place)
    across = (s, y * 2 + 1 - z)
    aside = core.other()
    pair = (s + 1 - 2 * par, y * 2 + 1 - z)

    def group(c):
        return (c // 2 * 2 + par, y * 2 + c % 2)

    def send(n, src, dst, to):
        return remote(src, dst, p_send.at[n], p_recv.at[n], to)

    barrier = pltpu.get_barrier_semaphore()

    def greet_head(d, carry):
        pl.semaphore_signal(barrier, inc=1, device_id=(s, (h + d) % NH), device_id_type=MESH)
        return carry

    def greet_seq(d, carry):
        pl.semaphore_signal(barrier, inc=1, device_id=group((g + d) % NS), device_id_type=MESH)
        return carry

    lax.fori_loop(1, NH, greet_head, 0)
    lax.fori_loop(1, NS, greet_seq, 0)
    for to in (aside, pair):
        pl.semaphore_signal(barrier, inc=1, device_id=to, device_id_type=MESH)

    pairs = (
        (tok_h, tok), (wk_h, wk), (m_in_h, m_in), (m_out_h, m_out), (wq_h, wq), (wv_h, wv), (ao_h, ao), (ak_h, ak), (av_h, av), (aq_h, aq),
    )
    loads = [pltpu.make_async_copy(src, dst, l_sem.at[n]) for n, (src, dst) in enumerate(pairs)]
    for load in loads:
        load.start()
    loads[0].wait()
    loads[1].wait()
    key = dot(tok[...], wk[...]).astype(BF16)
    kb[...] = key

    @pl.when(home)
    def _():
        kf[:, col(h)] = key

    hot = lax.broadcasted_iota(jnp.int32, (16, W), 0) == plan[0]

    def row(table):
        return jnp.sum(jnp.where(hot, table[...], 0.0), axis=0, keepdims=True)

    gown[...] = jnp.concatenate([row(mo), 1.0 - row(fg), row(st), jnp.zeros((5, W), F32)], axis=0)
    pl.semaphore_wait(barrier, NH - 1 + NS - 1 + 2)

    for load in loads[2:]:
        load.wait()
    ring_k = Ring(place, z, kf, g_send.at[0], g_recv.at[0])
    ring_q = Ring(place, z, qf, g_send.at[1], g_recv.at[1])
    ring_t = Ring(place, par, tf, g_send.at[2], g_recv.at[2])
    ring_c = Ring(place, z, cf, g_send.at[3], g_recv.at[3])

    x = s // 8

    def z_copy(n, c, src, dst):
        return send(n + c, src.at[half(c)], dst.at[half(c), col(h)], across)

    def side_rows(n, c, buf):
        return send(n + c, buf.at[half(c)], buf.at[half(c)], aside)

    def v_copy():
        return send(4, vb, vbuf, pair)

    def gate_copy():
        return send(5, gown, gates.at[s], pair)

    def mi_copy():
        ref = mi.at[pl.ds(pl.multiple_of(x * 256, 256), 256), :]
        return send(6, ref, ref, across)

    def mo_copy():
        ref = mob.at[pl.ds(pl.multiple_of(x * 32, 32), 32), :]
        return send(7, ref, ref, across)

    def share_copy(d, n):
        if n == 0:
            ref = mi.at[pl.ds(pl.multiple_of(x * 256, 256), 256), :]
        else:
            ref = mob.at[pl.ds(pl.multiple_of(x * 32, 32), 32), :]
        return remote(ref, ref, x_send.at[n, d - 1], x_recv.at[n, d - 1], ((x + d) % 4 * 8 + s % 8, h))

    def w0_copy():
        return send(8, w0s, w0, across)

    @pl.when(home)
    def _():
        for c in range(PARTS):
            ring_k.give_a(c)
        mi[...] = m_in[...].astype(BF16)
        mob[...] = m_out[...].astype(BF16)

    @pl.when(away)
    def _():
        for c in range(PARTS):
            z_copy(0, c, kb, kf).start()

    query = dot(tok[...], wq[...]).astype(BF16)
    qb[...] = query
    value = dot(tok[...], wv[...]).astype(BF16)

    @pl.when(home)
    def _():
        mi_copy().start()
        mo_copy().start()
        mot[...] = m_out[...].T
        qf[:, col(h)] = query
        vbuf[...] = value
        gates[g] = gown[...]

        def rows(c):
            r = pl.ds(pl.multiple_of(c * 32, 32), 32)
            return jnp.concatenate([m_in[r, :], mot[r, :]], axis=0)

        w0[...] = rows(g)
        w0s[...] = rows(g + 1 - 2 * z)
        w0_copy().start()

    @pl.when(away)
    def _():
        vb[...] = value
        v_copy().start()
        gate_copy().start()

    @pl.when(home)
    def _():
        for c in range(PARTS):
            z_copy(0, c, kb, kf).wait_recv()
            ring_k.give_b(c)
        for c in range(PARTS):
            ring_k.relay(c)
        for c in range(PARTS):
            ring_k.finish(c)
            side_rows(9, c, kf).start()

    @pl.when(away)
    def _():
        for n, copy in enumerate((mi_copy, mo_copy)):
            copy().wait_recv()
            for d in (2, 1, 3):
                share_copy(d, n).start()
        for n in range(2):
            for d in (1, 2, 3):
                share_copy(d, n).wait_recv()
        for c in range(PARTS):
            side_rows(9, c, kf).wait_recv()
        for c in range(PARTS):
            z_copy(2, c, qb, qf).start()

    pre = dot(kf[...], mi[...])
    sig = jax.nn.sigmoid(pre)
    hid[...] = (pre * sig).astype(BF16)
    slope[...] = sig * (1.0 + pre * (1.0 - sig))

    def part_one(c, b):
        return dot(hid[half(c), :], mob[:, col(b)])

    sum_one = Sum(core, part_one, rs_out.at[0], rs_land.at[0], r_send.at[0], r_recv.at[0])
    sum_one.run()

    @pl.when(away)
    def _():
        v_copy().wait_recv()
        gate_copy().wait_recv()
        w0_copy().wait_recv()

    own = core.y * 2 + par
    share_r = Share(core, rf, h_send, h_recv)
    for c in range(PARTS):
        rf[half(c), col(own)] = ((2.0 / T) * (sum_one.last(c) - vbuf[half(c), :].astype(F32))).astype(BF16)
        share_r.start(c)

    def send_gates(d, carry):
        remote(gates.at[g], gates.at[g], gt_send, gt_recv, group((g + d) % NS)).start()
        return carry

    lax.fori_loop(1, NS, send_gates, 0)
    kt[...] = kf[...].T
    for stage in (share_r.step, share_r.last, share_r.finish):
        for c in range(PARTS):
            stage(c)

    @pl.when(home)
    def _():
        for c in range(PARTS):
            ring_q.give_a(c)

    rate = gates[g][2:3]
    g_out = dot(hid[...].T, rf[...])
    gbuf[:, 32:64, :] = (g_out.T * -rate).astype(BF16).reshape(NS, 32, W)
    term = (dot(rf[...], mob[...], NT) * slope[...]).astype(BF16)
    gbuf[:, 0:32, :] = (dot(kt[...], term) * -rate).astype(BF16).reshape(NS, 32, W)

    def send_grad(d, carry):
        o = (g + d) % NS
        remote(gbuf.at[o], rbuf.at[g], a_send, a_recv.at[g], group(o)).start()
        return carry

    lax.fori_loop(1, NS, send_grad, 0)
    rbuf[g] = gbuf[g]

    def wo_copy(d):
        p = (h + d) % NH
        return remote(ao.at[:, col(p)], wo.at[pl.ds(pl.multiple_of(h * W, W), W), :], w_send.at[d - 1], w_recv.at[d - 1], (s, p))

    for d in range(1, NH):
        wo_copy(d).start()
    wo[pl.ds(pl.multiple_of(h * W, W), W), :] = ao[:, col(h)]

    pltpu.make_async_copy(gates.at[pl.ds(0, NS - 1)], gates.at[pl.ds(0, NS - 1)], gt_recv).wait()

    def step(c, carry):
        speed, weight = carry
        wbuf[c] = weight.astype(BF16)

        @pl.when(c != g)
        def _():
            remote(wbuf.at[c], wland.at[g], b_send, b_recv, group(c)).start()
            remote(gbuf.at[c], rbuf.at[c], a_send, a_recv.at[c], group(c)).wait_recv()

        gate = gates[c]
        speed = gate[0:1] * speed + rbuf[c].astype(F32)
        weight = gate[1:2] * weight + speed
        return speed, weight

    state = lax.fori_loop(0, 4, step, (jnp.zeros((64, W), F32), w0[...]))

    @pl.when(home)
    def _():
        for c in range(PARTS):
            z_copy(2, c, qb, qf).wait_recv()
            ring_q.give_b(c)

    state = lax.fori_loop(4, 20, step, state)

    @pl.when(home)
    def _():
        for c in range(PARTS):
            ring_q.relay(c)

    lax.fori_loop(20, NS, step, state)
    wland[g] = wbuf[g]
    @pl.when(home)
    def _():
        for c in range(PARTS):
            ring_q.finish(c)
            side_rows(11, c, qf).start()

    @pl.when(away)
    def _():
        for c in range(PARTS):
            side_rows(11, c, qf).wait_recv()

    some = pl.ds(0, NS - 1)
    pltpu.make_async_copy(wland.at[some], wland.at[some], b_recv).wait()

    act = dot(qf[...], wland[:, 0:32, :].reshape(1024, W))
    hq[...] = (act * jax.nn.sigmoid(act)).astype(BF16)

    def part_two(c, b):
        return dot(hq[half(c), :], wland[pl.ds(b * 4, 4), 32:64, :].reshape(W, W), NT)

    sum_two = Sum(core, part_two, rs_out.at[1], rs_land.at[1], r_send.at[1], r_recv.at[1])
    sum_two.run()

    def t_copy(n, c, to):
        return send(n + c, tb.at[half(c)], tf.at[half(c), col(own)], to)

    for c in range(PARTS):
        rows_c = sum_two.last(c).astype(BF16)
        tb[half(c), :] = rows_c

        @pl.when(home)
        def _():
            t_copy(13, c, across).start()
            tf[half(c), col(own)] = rows_c
            ring_t.give_a(c)

        @pl.when(away)
        def _():
            t_copy(15, c, pair).start()
            t_copy(17, c, aside).start()

    @pl.when(home)
    def _():
        for c in range(PARTS):
            t_copy(17, c, aside).wait_recv()
            ring_t.give_b(c)

    @pl.when(away)
    def _():
        for c in range(PARTS):
            t_copy(13, c, across).wait_recv()
            ring_t.give_a(c)
            t_copy(15, c, pair).wait_recv()
            ring_t.give_b(c)

    for c in range(PARTS):
        ring_t.relay(c)
    zl = (s // 2) % 4

    def hop(c, n, slot, to_slot, to):
        return remote(kv.at[slot, half(c)], kv.at[to_slot, half(c)], k_send.at[c, n], k_recv.at[c, to_slot], to)

    def own_copy(c, k):
        return hop(c, k, 0, 2 * k, (s + 2 * k, h))

    def side_copy(c):
        return hop(c, 0, 0, 1, (s + 1, h))

    def pass_copy(c, k):
        return hop(c, 4 + k, 2 * k, 2 * k + 1 - 2 * par, (s + 1 - 2 * par, h))

    def relay_copy(c, up):
        return hop(c, 9, 4, 6 if up else 2, (s + 2 if up else s - 2, h))

    def sends(k):
        ok = s + 2 * k < NS
        if k == 3:
            ok = ok & (zl != 0)
        if k == 1:
            ok = ok & (zl != 3)
        return ok

    def passes(k):
        return (s >= 2 * k) & ((par == 1) | (k < 4))

    for c in range(PARTS):
        ring_t.finish(c)
        for i in range(2):
            r = slice(c * HALF + i * 128, c * HALF + (i + 1) * 128)
            rows_i = tf[r, :].astype(F32)
            mean = jnp.mean(rows_i * rows_i, axis=-1, keepdims=True)
            nrm[r, :] = (rows_i * lax.rsqrt(mean + EPS) * gain[...]).astype(BF16)
        kv[0, half(c), 0:W] = dot(nrm[half(c), :], ak[...]).astype(BF16)
        kv[0, half(c), W : 2 * W] = dot(nrm[half(c), :], av[...]).astype(BF16)
        for k in (2, 1, 3, 4):

            @pl.when(sends(k))
            def _():
                own_copy(c, k).start()

        @pl.when(par == 0)
        def _():
            side_copy(c).start()

    query = dot(nrm[...], aq[...]).astype(BF16) * 0.125
    low = lax.broadcasted_iota(jnp.int32, (128, W), 1) < 64
    for i in range(4):
        part = query[i * 128 : (i + 1) * 128, :]
        qs[i, 0:128, :] = jnp.where(low, part, jnp.zeros_like(part))
        qs[i, 128:256, :] = jnp.where(low, jnp.zeros_like(part), part)
    m_s[...] = jnp.full_like(m_s, -1e30)
    acc[...] = jnp.zeros_like(acc)
    ones = jnp.ones((T, W), BF16)

    def attend(slot, mode, edge=None):
        values = jnp.concatenate([kv[slot, :, W : 2 * W], ones], axis=1)
        for i in range(4):
            sc = dot(qs[i], kv[slot, :, 0:W], NT)
            if mode != 1:
                iq = lax.broadcasted_iota(jnp.int32, (256, T), 0) % 128 + i * 128
                ik = lax.broadcasted_iota(jnp.int32, (256, T), 1)
                sc = jnp.where(iq >= ik if mode == 0 else ik - iq > edge, sc, -1e30)
            m_old = m_s[i]
            m_new = jnp.maximum(m_old, jnp.max(sc, axis=-1, keepdims=True))
            p = jnp.exp(sc - m_new)
            m_s[i] = m_new
            acc[i] = jnp.exp(m_old - m_new) * acc[i] + dot(p.astype(BF16), values)

    attend(0, 0)
    def arrive(c, slot):
        hop(c, 0, 0, slot, across).wait_recv()

    last = jnp.where(zl == 0, 1, 3)

    def chip(j):
        return jnp.where(j == 0, 2, jnp.where(j == 1, 4, jnp.where(j == 2, 4 - last, last)))

    def turn(j, carry):
        k = chip(j)
        odd = jnp.where(j == 0, par, 2 * chip(j - 1) - 1 + 2 * par)

        @pl.when((j < 4) & (s >= 2 * k))
        def _():
            for c in range(PARTS):
                arrive(c, 2 * k)

                @pl.when((k == 2) & (zl == 2))
                def _():
                    relay_copy(c, True).start()

                @pl.when((k == 2) & (zl == 1))
                def _():
                    relay_copy(c, False).start()

                @pl.when(passes(k))
                def _():
                    pass_copy(c, k).start()

            attend(2 * k, 2, jnp.where(k == 4, 0, -2 * T))

        @pl.when((odd > 0) & (odd < 9) & (s >= odd))
        def _():
            for c in range(PARTS):
                arrive(c, odd)
            attend(odd, 1)

        return carry

    lax.fori_loop(0, 5, turn, 0)
    for i in range(4):
        both = acc[i, :, 0:W] / acc[i, :, W : 2 * W]
        cf[i * 128 : (i + 1) * 128, col(h)] = jnp.where(low, both[0:128], both[128:256]).astype(BF16)

    def c_copy(c):
        ref = cf.at[half(c), col(h)]
        return send(19 + c, ref, ref, across)

    for c in range(PARTS):
        c_copy(c).start()
        ring_c.give_a(c)
    for c in range(PARTS):
        c_copy(c).wait_recv()
        ring_c.give_b(c)
    for d in range(1, NH):
        wo_copy(d).wait_recv()
    for c in range(PARTS):
        ring_c.relay(c)
    for c in range(PARTS):
        ring_c.finish(c)
        out_ref[half(c), :] = dot(cf[half(c), :], wo[...]).astype(BF16)

    @pl.when(home)
    def _():
        ring_k.drain()
        ring_q.drain()
        for c in range(PARTS):
            side_rows(9, c, kf).wait_send()
            side_rows(11, c, qf).wait_send()
            t_copy(13, c, across).wait_send()
        mi_copy().wait_send()
        mo_copy().wait_send()
        w0_copy().wait_send()

    @pl.when(away)
    def _():
        for c in range(PARTS):
            z_copy(0, c, kb, kf).wait_send()
            z_copy(2, c, qb, qf).wait_send()
            t_copy(17, c, aside).wait_send()
            t_copy(15, c, pair).wait_send()
        v_copy().wait_send()
        gate_copy().wait_send()
        for n in range(2):
            for d in (1, 2, 3):
                share_copy(d, n).wait_send()

    ring_t.drain()
    ring_c.drain()
    for c in range(PARTS):
        c_copy(c).wait_send()
    for group_copies in (sum_one, sum_two, share_r):
        group_copies.drain()
    for d in range(1, NH):
        wo_copy(d).wait_send()
    pltpu.make_async_copy(gates.at[some], gates.at[some], gt_send).wait()
    pltpu.make_async_copy(gbuf.at[some], gbuf.at[some], a_send).wait()
    pltpu.make_async_copy(wbuf.at[some], wbuf.at[some], b_send).wait()
    for c in range(PARTS):
        for k in range(1, 5):

            @pl.when(sends(k))
            def _():
                own_copy(c, k).wait_send()

            @pl.when(passes(k))
            def _():
                pass_copy(c, k).wait_send()

        @pl.when(par == 0)
        def _():
            side_copy(c).wait_send()

        @pl.when((s >= 4) & (zl == 2))
        def _():
            relay_copy(c, True).wait_send()

        @pl.when((s >= 4) & (zl == 1))
        def _():
            relay_copy(c, False).wait_send()


def block(
    tokens, mem_query_w, mem_key_w, mem_value_w, mem_in, mem_out, forget_levels, momentum_levels, step_levels,
    plan, norm_gain, attn_query_w, attn_key_w, attn_value_w, attn_out_w,
):
    vm = pl.BlockSpec(memory_space=pltpu.VMEM)
    sm = pl.BlockSpec(memory_space=pltpu.SMEM)
    hb = pl.BlockSpec(memory_space=pl.ANY)
    V = pltpu.VMEM
    dma = pltpu.SemaphoreType.DMA
    big = V((T, 1024), BF16)
    slab = V((NS, 64, W), BF16)
    return pl.pallas_call(
        kernel,
        name="titans",
        out_shape=jax.ShapeDtypeStruct((T, W), BF16),
        in_specs=[hb] * 6 + [vm] * 3 + [sm, vm] + [hb] * 4,
        out_specs=vm,
        scratch_shapes=[
            big, V((1024, W), BF16), V((1024, W), BF16), V((1024, W), BF16), V((1024, W), F32), V((W, 1024), F32),
            V((1024, W), BF16), V((1024, W), BF16), V((1024, W), BF16), V((W, 1024), BF16), dma((10,)),
            big, big, big, big, big,
            V((1024, W), BF16), V((T, W), BF16), V((T, W), BF16), V((T, W), BF16), V((T, W), BF16), V((T, W), BF16),
            V((T, W), BF16), V((T, W), F32), V((T, W), BF16), V((1024, W), BF16), V((W, 1024), BF16), V((1024, W), F32),
            V((64, W), F32), V((64, W), F32), V((1024, T), BF16),
            V((2, 7, T, W), BF16), V((2, 7, T, W), BF16), V((NS, 8, W), F32), V((8, W), F32),
            slab, slab, slab, slab,
            V((9, T, 2 * W), BF16), V((4, 256, W), BF16), big, V((4, 256, 1), F32), V((4, 256, 2 * W), F32),
            dma((4, PARTS, 6)), dma((4, PARTS, 6)), dma((PARTS, 7)), dma((PARTS, 7)), dma((2, PARTS, 7)), dma((2, PARTS, 7)), dma((21,)), dma((21,)),
            dma((7,)), dma((7,)), dma, dma,
            dma, dma((NS,)), dma, dma, dma((PARTS, 10)), dma((PARTS, 9)), dma((2, 3)), dma((2, 3)),
        ],
        compiler_params=pltpu.CompilerParams(collective_id=0, has_side_effects=True, vmem_limit_bytes=60 * 1024 * 1024),
    )(
        tokens, mem_query_w, mem_key_w, mem_value_w, mem_in, mem_out, forget_levels, momentum_levels, step_levels,
        plan, norm_gain.reshape(1, -1), attn_query_w, attn_key_w, attn_value_w, attn_out_w,
    )


def solution(mesh):
    seq, head = P("seq", None), P(None, "head")
    in_specs = (
        seq, head, head, head, head, P("head", None), head, head, head, P("seq"), P(), head, head, head, P("head", None),
    )
    return jax.shard_map(block, mesh=mesh, in_specs=in_specs, out_specs=P("seq", "head"), check_vma=False)
```

```python
import jax
import jax.numpy as jnp
from jax import lax
from jax.experimental import pallas as pl
from jax.experimental.pallas import tpu as pltpu
from jax.sharding import PartitionSpec as P

MESH = pl.DeviceIdType.MESH
F32 = jnp.float32
BF16 = jnp.bfloat16
EPS = 1e-06
NS = 32
NH = 8
T = 512
W = 128
NN = (((1,), (0,)), ((), ()))
NT = (((1,), (1,)), ((), ()))


def dot(a, b, dims=NN):
    return lax.dot_general(a, b, dims, preferred_element_type=F32)


def col(b):
    return pl.ds(pl.multiple_of(b * W, W), W)


def remote(src, dst, send, recv, device):
    return pltpu.make_async_remote_copy(
        src_ref=src, dst_ref=dst, send_sem=send, recv_sem=recv, device_id=device, device_id_type=MESH
    )


WINS = 2
PARTS = 4
HALF = T // PARTS


def half(c):
    return pl.ds(c * HALF, HALF)


def wait(ref, sem):
    pltpu.make_async_copy(ref, ref, sem).wait()


class Ring:
    def __init__(self, place, bit, buf, send, recv):
        self.s, self.y, self.z = place
        self.a, self.b = bit, 1 - bit
        self.buf, self.send, self.recv = buf, send, recv

    def copy(self, c, k):
        y, a, b = self.y, self.a, self.b
        up, down = (y + 1) % 4, (y + 3) % 4
        block, to = ((y * 2 + a, up), (y * 2 + a, down), (y * 2 + b, up), (y * 2 + b, down), (down * 2 + a, up), (up * 2 + b, down))[k]
        ref = self.buf.at[half(c), col(block)]
        return remote(ref, ref, self.send, self.recv.at[c, (0, 2, 2, 1, 2, 2)[k]], (self.s, to * 2 + self.z))

    def give_a(self, c):
        self.copy(c, 0).start()
        self.copy(c, 1).start()

    def give_b(self, c):
        self.copy(c, 2).start()
        self.copy(c, 3).start()

    def relay(self, c):
        self.copy(c, 0).wait_recv()
        self.copy(c, 4).start()
        self.copy(c, 3).wait_recv()
        self.copy(c, 5).start()

    def finish(self, c):
        wait(self.buf.at[half(c), pl.ds(0, 4 * W)], self.recv.at[c, 2])

    def drain(self):
        wait(self.buf.at[pl.ds(0, T * 6 // 8)], self.send)


class Core:
    def __init__(self, place):
        self.s, self.y, self.z = place
        self.k = self.s % 2
        up, down = (self.y + 1) % 4, (self.y + 3) % 4
        self.far = (self.y + 2) % 4
        self.next = jnp.where(self.k == 0, up, down)
        self.prev = jnp.where(self.k == 0, down, up)

    def at(self, y):
        return (self.s, y * 2 + self.z)

    def other(self):
        return (self.s + 1 - 2 * self.k, self.y * 2 + self.z)


class Share:
    def __init__(self, core, buf, send, recv):
        self.me, self.buf, self.send, self.recv = core, buf, send, recv

    def copy(self, c, n):
        me = self.me
        y = (me.y, me.y, me.prev, me.y, me.prev, me.next, me.far)[n]
        to = (me.at(me.next), me.at(me.prev), me.at(me.next), me.other(), me.other(), me.other(), me.other())[n]
        ref = self.buf.at[half(c), col(y * 2 + me.k)]
        return remote(ref, ref, self.send, self.recv.at[c, min(n, 3)], to)

    def start(self, c):
        for n in (0, 1, 3):
            self.copy(c, n).start()

    def step(self, c):
        self.copy(c, 0).wait_recv()
        self.copy(c, 2).start()
        self.copy(c, 4).start()
        self.copy(c, 1).wait_recv()
        self.copy(c, 5).start()

    def last(self, c):
        self.copy(c, 2).wait_recv()
        self.copy(c, 6).start()

    def finish(self, c):
        wait(self.buf.at[half(c), pl.ds(0, 4 * W)], self.recv.at[c, 3])

    def drain(self):
        wait(self.buf.at[pl.ds(0, T * 7 // 8)], self.send)


class Sum:
    def __init__(self, core, part, out, land, send, recv):
        self.me, self.part, self.out, self.land, self.send, self.recv = core, part, out, land, send, recv
        self.order = (core.far, core.next, core.prev, core.y)

    def copy(self, c, n):
        me = self.me
        to = me.other() if n < 4 else me.at(me.prev if n == 6 else me.next)
        return remote(self.out.at[n, half(c)], self.land.at[n, half(c)], self.send, self.recv.at[c, max(n - 3, 0)], to)

    def put(self, c, n, value):
        self.out[n, half(c), :] = value.astype(BF16)
        self.copy(c, n).start()

    def got(self, c, n):
        self.copy(c, n).wait_recv()
        return self.land[n, half(c), :].astype(F32)

    def give(self, c):
        for n, y in enumerate(self.order):
            self.put(c, n, self.part(c, y * 2 + 1 - self.me.k))

    def chip(self, c, n):
        return self.part(c, self.order[n] * 2 + self.me.k) + self.land[(0, 2, 1, 3)[n], half(c), :].astype(F32)

    def first(self, c):
        wait(self.land.at[pl.ds(0, 4), half(c)], self.recv.at[c, 0])
        self.put(c, 4, self.chip(c, 0))
        self.put(c, 6, self.chip(c, 2))

    def second(self, c):
        onward = self.chip(c, 1)
        self.put(c, 5, self.got(c, 4) + onward)

    def last(self, c):
        own = self.chip(c, 3)
        return own + self.got(c, 6) + self.got(c, 5)

    def run(self):
        for stage in (self.give, self.first, self.second):
            for c in range(PARTS):
                stage(c)

    def drain(self):
        wait(self.out, self.send)


def kernel(
    tok_h, wq_h, wk_h, wv_h, m_in_h, m_out_h, fg, mo, st, plan, gain, aq_h, ak_h, av_h, ao_h, out_ref,
    tok, wk, wq, wv, m_in, m_out, aq, ak, av, ao, l_sem, ob, o_sem,
    kf, qf, rf, tf, cf, wo, kb, qb, vb, tb, vbuf, hid, slope, hq, mi, mob, mot, w0, w0s, kt,
    rs_out, rs_land, gates, gown, gbuf, rbuf, wbuf, wland, kv, qs, nrm, m_s, acc,
    g_send, g_recv, h_send, h_recv, r_send, r_recv, p_send, p_recv, q_recv, w_send, w_recv, gt_send, gt_recv,
    a_send, a_recv, b_send, b_recv, k_send, k_recv, x_send, x_recv,
):
    s, h = lax.axis_index("seq"), lax.axis_index("head")
    y, z = h // 2, h % 2
    place = (s, y, z)
    par = s % 2
    home = par == z
    away = par != z
    g = s - par + z
    core = Core(place)
    across = (s, y * 2 + 1 - z)
    aside = core.other()
    pair = (s + 1 - 2 * par, y * 2 + 1 - z)

    def group(c):
        return (c // 2 * 2 + par, y * 2 + c % 2)

    def send(n, src, dst, to, c=0):
        return remote(src, dst, p_send.at[n], p_recv.at[n * PARTS + c] if n < 6 else q_recv.at[n - 6], to)

    barrier = pltpu.get_barrier_semaphore()

    def greet_head(d, carry):
        pl.semaphore_signal(barrier, inc=1, device_id=(s, (h + d) % NH), device_id_type=MESH)
        return carry

    def greet_seq(d, carry):
        pl.semaphore_signal(barrier, inc=1, device_id=group((g + d) % NS), device_id_type=MESH)
        return carry

    lax.fori_loop(1, NH, greet_head, 0)
    lax.fori_loop(1, NS, greet_seq, 0)
    for to in (aside, pair):
        pl.semaphore_signal(barrier, inc=1, device_id=to, device_id_type=MESH)

    pairs = (
        (tok_h, tok), (wk_h, wk), (m_in_h, m_in), (m_out_h, m_out), (wq_h, wq), (wv_h, wv), (ao_h, ao), (ak_h, ak), (av_h, av), (aq_h, aq),
    )
    loads = [pltpu.make_async_copy(src, dst, l_sem.at[n]) for n, (src, dst) in enumerate(pairs)]
    for load in loads:
        load.start()
    loads[0].wait()
    loads[1].wait()
    key = dot(tok[...], wk[...]).astype(BF16)
    kb[...] = key

    @pl.when(home)
    def _():
        kf[:, col(h)] = key

    hot = lax.broadcasted_iota(jnp.int32, (16, W), 0) == plan[0]

    def row(table):
        return jnp.sum(jnp.where(hot, table[...], 0.0), axis=0, keepdims=True)

    gown[...] = jnp.concatenate([row(mo), 1.0 - row(fg), row(st), jnp.zeros((5, W), F32)], axis=0)
    pl.semaphore_wait(barrier, NH - 1 + NS - 1 + 2)

    for load in loads[2:]:
        load.wait()
    ring_k = Ring(place, z, kf, g_send.at[0], g_recv.at[0])
    ring_q = Ring(place, z, qf, g_send.at[1], g_recv.at[1])
    ring_t = Ring(place, par, tf, g_send.at[2], g_recv.at[2])
    ring_c = Ring(place, z, cf, g_send.at[3], g_recv.at[3])

    x = s // 8

    def z_copy(n, c, src, dst):
        return send(n, src.at[half(c)], dst.at[half(c), col(h)], across, c)

    def side_rows(n, c, buf):
        return send(n, buf.at[half(c)], buf.at[half(c)], aside, c)

    def v_copy():
        return send(8, vb, vbuf, pair)

    def gate_copy():
        return send(9, gown, gates.at[s], pair)

    def mi_copy():
        ref = mi.at[pl.ds(pl.multiple_of(x * 256, 256), 256), :]
        return send(10, ref, ref, across)

    def mo_copy():
        ref = mob.at[pl.ds(pl.multiple_of(x * 32, 32), 32), :]
        return send(11, ref, ref, across)

    def share_copy(d, n):
        if n == 0:
            ref = mi.at[pl.ds(pl.multiple_of(x * 256, 256), 256), :]
        else:
            ref = mob.at[pl.ds(pl.multiple_of(x * 32, 32), 32), :]
        return remote(ref, ref, x_send, x_recv.at[n], ((x + d) % 4 * 8 + s % 8, h))

    def w0_copy():
        return send(12, w0s, w0, across)

    @pl.when(home)
    def _():
        for c in range(PARTS):
            ring_k.give_a(c)
        mi[...] = m_in[...].astype(BF16)
        mob[...] = m_out[...].astype(BF16)

    @pl.when(away)
    def _():
        for c in range(PARTS):
            z_copy(0, c, kb, kf).start()

    query = dot(tok[...], wq[...]).astype(BF16)
    qb[...] = query
    value = dot(tok[...], wv[...]).astype(BF16)

    @pl.when(home)
    def _():
        mi_copy().start()
        mo_copy().start()
        mot[...] = m_out[...].T
        qf[:, col(h)] = query
        vbuf[...] = value
        gates[g] = gown[...]

        def rows(c):
            r = pl.ds(pl.multiple_of(c * 32, 32), 32)
            return jnp.concatenate([m_in[r, :], mot[r, :]], axis=0)

        w0[...] = rows(g)
        w0s[...] = rows(g + 1 - 2 * z)
        w0_copy().start()

    @pl.when(away)
    def _():
        vb[...] = value
        v_copy().start()
        gate_copy().start()

    @pl.when(home)
    def _():
        for c in range(PARTS):
            z_copy(0, c, kb, kf).wait_recv()
            ring_k.give_b(c)
        for c in range(PARTS):
            ring_k.relay(c)
        for c in range(PARTS):
            ring_k.finish(c)
            side_rows(1, c, kf).start()

    @pl.when(away)
    def _():
        for n, copy in enumerate((mi_copy, mo_copy)):
            copy().wait_recv()
            for d in (2, 1, 3):
                share_copy(d, n).start()
        wait(mi.at[pl.ds(0, 768)], x_recv.at[0])
        wait(mob.at[pl.ds(0, 96)], x_recv.at[1])
        for c in range(PARTS):
            side_rows(1, c, kf).wait_recv()
        for c in range(PARTS):
            z_copy(6, c, qb, qf).start()

    pre = dot(kf[...], mi[...])
    sig = jax.nn.sigmoid(pre)
    hid[...] = (pre * sig).astype(BF16)
    slope[...] = sig * (1.0 + pre * (1.0 - sig))

    def part_one(c, b):
        return dot(hid[half(c), :], mob[:, col(b)])

    sum_one = Sum(core, part_one, rs_out.at[0], rs_land.at[0], r_send.at[0], r_recv.at[0])
    sum_one.run()

    @pl.when(away)
    def _():
        v_copy().wait_recv()
        gate_copy().wait_recv()
        w0_copy().wait_recv()

    own = core.y * 2 + par
    share_r = Share(core, rf, h_send, h_recv)
    for c in range(PARTS):
        rf[half(c), col(own)] = ((2.0 / T) * (sum_one.last(c) - vbuf[half(c), :].astype(F32))).astype(BF16)
        share_r.start(c)

    def send_gates(d, carry):
        remote(gates.at[g], gates.at[g], gt_send, gt_recv, group((g + d) % NS)).start()
        return carry

    lax.fori_loop(1, NS, send_gates, 0)
    kt[...] = kf[...].T
    for stage in (share_r.step, share_r.last, share_r.finish):
        for c in range(PARTS):
            stage(c)

    @pl.when(home)
    def _():
        for c in range(PARTS):
            ring_q.give_a(c)

    rate = gates[g][2:3]
    g_out = dot(hid[...].T, rf[...])
    gbuf[:, 32:64, :] = (g_out.T * -rate).astype(BF16).reshape(NS, 32, W)
    term = (dot(rf[...], mob[...], NT) * slope[...]).astype(BF16)
    gbuf[:, 0:32, :] = (dot(kt[...], term) * -rate).astype(BF16).reshape(NS, 32, W)

    def send_grad(d, carry):
        o = (g + d) % NS
        remote(gbuf.at[o], rbuf.at[g], a_send, a_recv.at[g], group(o)).start()
        return carry

    lax.fori_loop(1, NS, send_grad, 0)
    rbuf[g] = gbuf[g]

    def wo_copy(d):
        p = (h + d) % NH
        return remote(ao.at[:, col(p)], wo.at[pl.ds(pl.multiple_of(h * W, W), W), :], w_send, w_recv, (s, p))

    for d in range(1, NH):
        wo_copy(d).start()
    wo[pl.ds(pl.multiple_of(h * W, W), W), :] = ao[:, col(h)]

    pltpu.make_async_copy(gates.at[pl.ds(0, NS - 1)], gates.at[pl.ds(0, NS - 1)], gt_recv).wait()

    def step(c, carry):
        speed, weight = carry
        wbuf[c] = weight.astype(BF16)

        @pl.when(c != g)
        def _():
            remote(wbuf.at[c], wland.at[g], b_send, b_recv, group(c)).start()
            remote(gbuf.at[c], rbuf.at[c], a_send, a_recv.at[c], group(c)).wait_recv()

        gate = gates[c]
        speed = gate[0:1] * speed + rbuf[c].astype(F32)
        weight = gate[1:2] * weight + speed
        return speed, weight

    state = lax.fori_loop(0, 4, step, (jnp.zeros((64, W), F32), w0[...]))

    @pl.when(home)
    def _():
        wait(qb, q_recv.at[0])
        for c in range(PARTS):
            ring_q.give_b(c)

    state = lax.fori_loop(4, 20, step, state)

    @pl.when(home)
    def _():
        for c in range(PARTS):
            ring_q.relay(c)

    lax.fori_loop(20, NS, step, state)
    wland[g] = wbuf[g]
    @pl.when(home)
    def _():
        for c in range(PARTS):
            ring_q.finish(c)
            side_rows(7, c, qf).start()

    @pl.when(away)
    def _():
        wait(qf, q_recv.at[1])

    some = pl.ds(0, NS - 1)
    pltpu.make_async_copy(wland.at[some], wland.at[some], b_recv).wait()

    act = dot(qf[...], wland[:, 0:32, :].reshape(1024, W))
    hq[...] = (act * jax.nn.sigmoid(act)).astype(BF16)

    def part_two(c, b):
        return dot(hq[half(c), :], wland[pl.ds(b * 4, 4), 32:64, :].reshape(W, W), NT)

    sum_two = Sum(core, part_two, rs_out.at[1], rs_land.at[1], r_send.at[1], r_recv.at[1])
    sum_two.run()

    def t_copy(n, c, to):
        return send(n, tb.at[half(c)], tf.at[half(c), col(own)], to, c)

    for c in range(PARTS):
        rows_c = sum_two.last(c).astype(BF16)
        tb[half(c), :] = rows_c

        @pl.when(home)
        def _():
            t_copy(2, c, across).start()
            tf[half(c), col(own)] = rows_c
            ring_t.give_a(c)

        @pl.when(away)
        def _():
            t_copy(3, c, pair).start()
            t_copy(4, c, aside).start()

    @pl.when(home)
    def _():
        for c in range(PARTS):
            t_copy(4, c, aside).wait_recv()
            ring_t.give_b(c)

    @pl.when(away)
    def _():
        for c in range(PARTS):
            t_copy(2, c, across).wait_recv()
            ring_t.give_a(c)
            t_copy(3, c, pair).wait_recv()
            ring_t.give_b(c)

    for c in range(PARTS):
        ring_t.relay(c)
    zl = (s // 2) % 4

    def hop(c, n, slot, to_slot, to):
        r = pl.ds(c * (T // WINS), T // WINS)
        return remote(kv.at[slot, r], kv.at[to_slot, r], k_send.at[n], k_recv.at[c, to_slot], to)

    def own_copy(c, k):
        return hop(c, k, 0, 2 * k, (s + 2 * k, h))

    def side_copy(c):
        return hop(c, 0, 0, 1, (s + 1, h))

    def pass_copy(c, k):
        return hop(c, 4 + k, 2 * k, 2 * k + 1 - 2 * par, (s + 1 - 2 * par, h))

    def relay_copy(c, up):
        return hop(c, 9, 4, 6 if up else 2, (s + 2 if up else s - 2, h))

    def sends(k):
        ok = s + 2 * k < NS
        if k == 3:
            ok = ok & (zl != 0)
        if k == 1:
            ok = ok & (zl != 3)
        return ok

    def passes(k):
        return (s >= 2 * k) & ((par == 1) | (k < 4))

    for c in range(PARTS):
        ring_t.finish(c)
        for i in range(HALF // 128):
            r = slice(c * HALF + i * 128, c * HALF + (i + 1) * 128)
            rows_i = tf[r, :].astype(F32)
            mean = jnp.mean(rows_i * rows_i, axis=-1, keepdims=True)
            nrm[r, :] = (rows_i * lax.rsqrt(mean + EPS) * gain[...]).astype(BF16)
        kv[0, half(c), 0:W] = dot(nrm[half(c), :], ak[...]).astype(BF16)
        kv[0, half(c), W : 2 * W] = dot(nrm[half(c), :], av[...]).astype(BF16)
        if (c + 1) % (PARTS // WINS) == 0:
            w = (c + 1) // (PARTS // WINS) - 1
            for k in (2, 1, 3, 4):

                @pl.when(sends(k))
                def _():
                    own_copy(w, k).start()

            @pl.when(par == 0)
            def _():
                side_copy(w).start()

    query = dot(nrm[...], aq[...]).astype(BF16) * 0.125
    low = lax.broadcasted_iota(jnp.int32, (128, W), 1) < 64
    for i in range(4):
        part = query[i * 128 : (i + 1) * 128, :]
        qs[i, 0:128, :] = jnp.where(low, part, jnp.zeros_like(part))
        qs[i, 128:256, :] = jnp.where(low, jnp.zeros_like(part), part)
    m_s[...] = jnp.full_like(m_s, -1e30)
    acc[...] = jnp.zeros_like(acc)
    ones = jnp.ones((T, W), BF16)

    def attend(slot, mode, edge=None):
        values = jnp.concatenate([kv[slot, :, W : 2 * W], ones], axis=1)
        for i in range(4):
            sc = dot(qs[i], kv[slot, :, 0:W], NT)
            if mode != 1:
                iq = lax.broadcasted_iota(jnp.int32, (256, T), 0) % 128 + i * 128
                ik = lax.broadcasted_iota(jnp.int32, (256, T), 1)
                sc = jnp.where(iq >= ik if mode == 0 else ik - iq > edge, sc, -1e30)
            m_old = m_s[i]
            m_new = jnp.maximum(m_old, jnp.max(sc, axis=-1, keepdims=True))
            p = jnp.exp(sc - m_new)
            m_s[i] = m_new
            acc[i] = jnp.exp(m_old - m_new) * acc[i] + dot(p.astype(BF16), values)

    attend(0, 0)
    def arrive(c, slot):
        hop(c, 0, 0, slot, across).wait_recv()

    last = jnp.where(zl == 0, 1, 3)

    def chip(j):
        return jnp.where(j == 0, 2, jnp.where(j == 1, 4, jnp.where(j == 2, 4 - last, last)))

    def turn(j, carry):
        k = chip(j)
        odd = jnp.where(j == 0, par, 2 * chip(j - 1) - 1 + 2 * par)

        @pl.when((j < 4) & (s >= 2 * k))
        def _():
            for c in range(WINS):
                arrive(c, 2 * k)

                @pl.when((k == 2) & (zl == 2))
                def _():
                    relay_copy(c, True).start()

                @pl.when((k == 2) & (zl == 1))
                def _():
                    relay_copy(c, False).start()

                @pl.when(passes(k))
                def _():
                    pass_copy(c, k).start()

            attend(2 * k, 2, jnp.where(k == 4, 0, -2 * T))

        @pl.when((odd > 0) & (odd < 9) & (s >= odd))
        def _():
            for c in range(WINS):
                arrive(c, odd)
            attend(odd, 1)

        return carry

    lax.fori_loop(0, 5, turn, 0)
    for i in range(4):
        both = acc[i, :, 0:W] / acc[i, :, W : 2 * W]
        cf[i * 128 : (i + 1) * 128, col(h)] = jnp.where(low, both[0:128], both[128:256]).astype(BF16)

    def out_copy(c):
        return pltpu.make_async_copy(ob.at[half(c)], out_ref.at[half(c)], o_sem.at[c])

    def c_copy(c):
        ref = cf.at[half(c), col(h)]
        return send(5, ref, ref, across, c)

    for c in range(PARTS):
        c_copy(c).start()
        ring_c.give_a(c)
    for c in range(PARTS):
        c_copy(c).wait_recv()
        ring_c.give_b(c)
    wait(wo.at[pl.ds(0, 7 * W)], w_recv)
    for c in range(PARTS):
        ring_c.relay(c)
    for c in range(PARTS):
        ring_c.finish(c)
        ob[half(c), :] = dot(cf[half(c), :], wo[...]).astype(BF16)
        out_copy(c).start()

    @pl.when(home)
    def _():
        ring_k.drain()
        ring_q.drain()
        wait(kf, p_send.at[1])
        wait(qf, p_send.at[7])
        wait(tb, p_send.at[2])
        mi_copy().wait_send()
        mo_copy().wait_send()
        w0_copy().wait_send()

    @pl.when(away)
    def _():
        wait(kb, p_send.at[0])
        wait(qb, p_send.at[6])
        wait(tb, p_send.at[3])
        wait(tb, p_send.at[4])
        v_copy().wait_send()
        gate_copy().wait_send()
        wait(kf.at[pl.ds(0, 192)], x_send)

    ring_t.drain()
    ring_c.drain()
    wait(kb, p_send.at[5])
    for c in range(PARTS):
        out_copy(c).wait()
    for group_copies in (sum_one, sum_two, share_r):
        group_copies.drain()
    wait(wo.at[pl.ds(0, 7 * W)], w_send)
    pltpu.make_async_copy(gates.at[some], gates.at[some], gt_send).wait()
    pltpu.make_async_copy(gbuf.at[some], gbuf.at[some], a_send).wait()
    pltpu.make_async_copy(wbuf.at[some], wbuf.at[some], b_send).wait()
    for k in range(1, 5):

        @pl.when(sends(k))
        def _():
            wait(kv.at[0], k_send.at[k])

        @pl.when(passes(k))
        def _():
            wait(kv.at[0], k_send.at[4 + k])

    @pl.when(par == 0)
    def _():
        wait(kv.at[0], k_send.at[0])

    @pl.when((s >= 4) & ((zl == 1) | (zl == 2)))
    def _():
        wait(kv.at[0], k_send.at[9])


def block(
    tokens, mem_query_w, mem_key_w, mem_value_w, mem_in, mem_out, forget_levels, momentum_levels, step_levels,
    plan, norm_gain, attn_query_w, attn_key_w, attn_value_w, attn_out_w,
):
    vm = pl.BlockSpec(memory_space=pltpu.VMEM)
    sm = pl.BlockSpec(memory_space=pltpu.SMEM)
    hb = pl.BlockSpec(memory_space=pl.ANY)
    V = pltpu.VMEM
    dma = pltpu.SemaphoreType.DMA
    big = V((T, 1024), BF16)
    slab = V((NS, 64, W), BF16)
    return pl.pallas_call(
        kernel,
        name="titans",
        out_shape=jax.ShapeDtypeStruct((T, W), BF16),
        in_specs=[hb] * 6 + [vm] * 3 + [sm, vm] + [hb] * 4,
        out_specs=hb,
        scratch_shapes=[
            big, V((1024, W), BF16), V((1024, W), BF16), V((1024, W), BF16), V((1024, W), F32), V((W, 1024), F32),
            V((1024, W), BF16), V((1024, W), BF16), V((1024, W), BF16), V((W, 1024), BF16), dma((10,)), V((T, W), BF16), dma((PARTS,)),
            big, big, big, big, big,
            V((1024, W), BF16), V((T, W), BF16), V((T, W), BF16), V((T, W), BF16), V((T, W), BF16), V((T, W), BF16),
            V((T, W), BF16), V((T, W), F32), V((T, W), BF16), V((1024, W), BF16), V((W, 1024), BF16), V((1024, W), F32),
            V((64, W), F32), V((64, W), F32), V((1024, T), BF16),
            V((2, 7, T, W), BF16), V((2, 7, T, W), BF16), V((NS, 8, W), F32), V((8, W), F32),
            slab, slab, slab, slab,
            V((9, T, 2 * W), BF16), V((4, 256, W), BF16), big, V((4, 256, 1), F32), V((4, 256, 2 * W), F32),
            dma((4,)), dma((4, PARTS, 3)), dma, dma((PARTS, 4)), dma((2,)), dma((2, PARTS, 4)), dma((13,)), dma((6 * PARTS,)), dma((7,)),
            dma, dma, dma, dma,
            dma, dma((NS,)), dma, dma, dma((10,)), dma((WINS, 9)), dma, dma((2,)),
        ],
        compiler_params=pltpu.CompilerParams(collective_id=0, has_side_effects=True, vmem_limit_bytes=60 * 1024 * 1024),
    )(
        tokens, mem_query_w, mem_key_w, mem_value_w, mem_in, mem_out, forget_levels, momentum_levels, step_levels,
        plan, norm_gain.reshape(1, -1), attn_query_w, attn_key_w, attn_value_w, attn_out_w,
    )


def solution(mesh):
    seq, head = P("seq", None), P(None, "head")
    in_specs = (
        seq, head, head, head, head, P("head", None), head, head, head, P("seq"), P(), head, head, head, P("head", None),
    )
    return jax.shard_map(block, mesh=mesh, in_specs=in_specs, out_specs=P("seq", "head"), check_vma=False)
```

```python
import jax
import jax.numpy as jnp
from jax import lax
from jax.experimental import pallas as pl
from jax.experimental.pallas import tpu as pltpu
from jax.sharding import PartitionSpec as P

MESH = pl.DeviceIdType.MESH
F32 = jnp.float32
BF16 = jnp.bfloat16
EPS = 1e-06
NS = 32
NH = 8
T = 512
W = 128
NN = (((1,), (0,)), ((), ()))
NT = (((1,), (1,)), ((), ()))


def dot(a, b, dims=NN):
    return lax.dot_general(a, b, dims, preferred_element_type=F32)


def col(b):
    return pl.ds(pl.multiple_of(b * W, W), W)


def remote(src, dst, send, recv, device):
    return pltpu.make_async_remote_copy(
        src_ref=src, dst_ref=dst, send_sem=send, recv_sem=recv, device_id=device, device_id_type=MESH
    )


WINS = 2
PARTS = 4
HALF = T // PARTS


def half(c):
    return pl.ds(c * HALF, HALF)


def wait(ref, sem):
    pltpu.make_async_copy(ref, ref, sem).wait()


class Ring:
    def __init__(self, place, bit, buf, send, recv):
        self.s, self.y, self.z = place
        self.a, self.b = bit, 1 - bit
        self.buf, self.send, self.recv = buf, send, recv

    def copy(self, c, k):
        y, a, b = self.y, self.a, self.b
        up, down = (y + 1) % 4, (y + 3) % 4
        block, to = ((y * 2 + a, up), (y * 2 + a, down), (y * 2 + b, up), (y * 2 + b, down), (down * 2 + a, up), (up * 2 + b, down))[k]
        ref = self.buf.at[half(c), col(block)]
        return remote(ref, ref, self.send, self.recv.at[c, (0, 2, 2, 1, 2, 2)[k]], (self.s, to * 2 + self.z))

    def give_a(self, c):
        self.copy(c, 0).start()
        self.copy(c, 1).start()

    def give_b(self, c):
        self.copy(c, 2).start()
        self.copy(c, 3).start()

    def relay(self, c):
        self.copy(c, 0).wait_recv()
        self.copy(c, 4).start()
        self.copy(c, 3).wait_recv()
        self.copy(c, 5).start()

    def finish(self, c):
        wait(self.buf.at[half(c), pl.ds(0, 4 * W)], self.recv.at[c, 2])

    def drain(self):
        wait(self.buf.at[pl.ds(0, T * 6 // 8)], self.send)


class Core:
    def __init__(self, place):
        self.s, self.y, self.z = place
        self.k = self.s % 2
        up, down = (self.y + 1) % 4, (self.y + 3) % 4
        self.far = (self.y + 2) % 4
        self.next = jnp.where(self.k == 0, up, down)
        self.prev = jnp.where(self.k == 0, down, up)

    def at(self, y):
        return (self.s, y * 2 + self.z)

    def other(self):
        return (self.s + 1 - 2 * self.k, self.y * 2 + self.z)


class Share:
    def __init__(self, core, ref, four, seven, send, recv):
        self.me, self.ref, self.four, self.seven, self.send, self.recv = core, ref, four, seven, send, recv

    def copy(self, c, n):
        me = self.me
        y = (me.y, me.y, me.prev, me.y, me.prev, me.next, me.far)[n]
        to = (me.at(me.next), me.at(me.prev), me.at(me.next), me.other(), me.other(), me.other(), me.other())[n]
        ref = self.ref(c, y * 2 + me.k)
        return remote(ref, ref, self.send, self.recv.at[c, min(n, 3)], to)

    def start(self, c):
        for n in (0, 1, 3):
            self.copy(c, n).start()

    def step(self, c):
        self.copy(c, 0).wait_recv()
        self.copy(c, 2).start()
        self.copy(c, 4).start()
        self.copy(c, 1).wait_recv()
        self.copy(c, 5).start()

    def last(self, c):
        self.copy(c, 2).wait_recv()
        self.copy(c, 6).start()

    def finish(self, c):
        wait(self.four(c), self.recv.at[c, 3])

    def drain(self):
        wait(self.seven, self.send)


class Sum:
    def __init__(self, core, part, out, land, send, recv):
        self.me, self.part, self.out, self.land, self.send, self.recv = core, part, out, land, send, recv
        self.order = (core.far, core.next, core.prev, core.y)

    def copy(self, c, n):
        me = self.me
        to = me.other() if n < 4 else me.at(me.prev if n == 6 else me.next)
        return remote(self.out.at[n, half(c)], self.land.at[n, half(c)], self.send, self.recv.at[c, max(n - 3, 0)], to)

    def put(self, c, n, value):
        self.out[n, half(c), :] = value.astype(BF16)
        self.copy(c, n).start()

    def got(self, c, n):
        self.copy(c, n).wait_recv()
        return self.land[n, half(c), :].astype(F32)

    def give(self, c):
        for n, y in enumerate(self.order):
            self.put(c, n, self.part(c, y * 2 + 1 - self.me.k))

    def chip(self, c, n):
        return self.part(c, self.order[n] * 2 + self.me.k) + self.land[(0, 2, 1, 3)[n], half(c), :].astype(F32)

    def first(self, c):
        wait(self.land.at[pl.ds(0, 4), half(c)], self.recv.at[c, 0])
        self.put(c, 4, self.chip(c, 0))
        self.put(c, 6, self.chip(c, 2))

    def second(self, c):
        onward = self.chip(c, 1)
        self.put(c, 5, self.got(c, 4) + onward)

    def last(self, c):
        own = self.chip(c, 3)
        return own + self.got(c, 6) + self.got(c, 5)

    def run(self):
        for stage in (self.give, self.first, self.second):
            for c in range(PARTS):
                stage(c)

    def drain(self):
        wait(self.out, self.send)


def kernel(
    tok_h, wq_h, wk_h, wv_h, m_in_h, m_out_h, fg, mo, st, plan, gain, aq_h, ak_h, av_h, ao_h, out_ref,
    tok, wk, wq, wv, m_in, m_out, aq, ak, av, ao, l_sem, ob, o_sem,
    kf, qf, rf, tf, cf, hf, vf, wo, kb, qb, vb, tb, slope, hq, mi, mof, mot, w0, w0s, kt,
    rs_out, rs_land, gates, gown, gbuf, rbuf, wbuf, wland, kv, qs, nrm, m_s, acc,
    g_send, g_recv, f_send, f_recv, h_send, h_recv, r_send, r_recv, p_send, p_recv, q_recv, w_send, w_recv, gt_send, gt_recv,
    a_send, a_recv, b_send, b_recv, k_send, k_recv, x_send, x_recv,
):
    s, h = lax.axis_index("seq"), lax.axis_index("head")
    y, z = h // 2, h % 2
    place = (s, y, z)
    par = s % 2
    home = par == z
    away = par != z
    g = s - par + z
    core = Core(place)
    across = (s, y * 2 + 1 - z)
    aside = core.other()
    pair = (s + 1 - 2 * par, y * 2 + 1 - z)

    def group(c):
        return (c // 2 * 2 + par, y * 2 + c % 2)

    def send(n, src, dst, to, c=0):
        return remote(src, dst, p_send.at[n], p_recv.at[n * PARTS + c] if n < 6 else q_recv.at[n - 6], to)

    barrier = pltpu.get_barrier_semaphore()

    def greet_head(d, carry):
        pl.semaphore_signal(barrier, inc=1, device_id=(s, (h + d) % NH), device_id_type=MESH)
        return carry

    def greet_seq(d, carry):
        pl.semaphore_signal(barrier, inc=1, device_id=group((g + d) % NS), device_id_type=MESH)
        return carry

    lax.fori_loop(1, NH, greet_head, 0)
    lax.fori_loop(1, NS, greet_seq, 0)
    for to in (aside, pair):
        pl.semaphore_signal(barrier, inc=1, device_id=to, device_id_type=MESH)

    pairs = (
        (tok_h, tok), (wk_h, wk), (m_in_h, m_in), (m_out_h, m_out), (wq_h, wq), (wv_h, wv), (ao_h, ao), (ak_h, ak), (av_h, av), (aq_h, aq),
    )
    loads = [pltpu.make_async_copy(src, dst, l_sem.at[n]) for n, (src, dst) in enumerate(pairs)]
    for load in loads:
        load.start()
    loads[0].wait()
    loads[1].wait()
    key = dot(tok[...], wk[...]).astype(BF16)
    kb[...] = key

    @pl.when(home)
    def _():
        kf[:, col(h)] = key

    hot = lax.broadcasted_iota(jnp.int32, (16, W), 0) == plan[0]

    def row(table):
        return jnp.sum(jnp.where(hot, table[...], 0.0), axis=0, keepdims=True)

    gown[...] = jnp.concatenate([row(mo), 1.0 - row(fg), row(st), jnp.zeros((5, W), F32)], axis=0)
    pl.semaphore_wait(barrier, NH - 1 + NS - 1 + 2)

    for load in loads[2:]:
        load.wait()
    ring_k = Ring(place, z, kf, g_send.at[0], g_recv.at[0])
    ring_q = Ring(place, z, qf, g_send.at[1], g_recv.at[1])
    ring_t = Ring(place, par, tf, g_send.at[2], g_recv.at[2])
    ring_c = Ring(place, z, cf, g_send.at[3], g_recv.at[3])
    ring_v = Ring(place, z, vf, g_send.at[4], g_recv.at[4])
    own = y * 2 + par

    def cols_of(buf):
        return (lambda c, b: buf.at[half(c), col(b)], lambda c: buf.at[half(c), pl.ds(0, 4 * W)], buf.at[pl.ds(0, T * 7 // 8)])

    share_h = Share(core, *cols_of(hf), h_send, h_recv)
    share_m = Share(core, lambda c, b: mof.at[col(b)], lambda c: mof.at[pl.ds(0, 4 * W)], mof.at[pl.ds(0, 7 * W)], f_send, f_recv)

    x = s // 8

    def z_copy(n, c, src, dst):
        return send(n, src.at[half(c)], dst.at[half(c), col(h)], across, c)

    def side_rows(n, c, buf):
        return send(n, buf.at[half(c)], buf.at[half(c)], aside, c)

    def gate_copy():
        return send(13, gown, gates.at[s], pair)

    def mi_copy():
        ref = mi.at[pl.ds(pl.multiple_of(x * 256, 256), 256), :]
        return send(10, ref, ref, across)

    def mo_copy():
        ref = mof.at[pl.ds(pl.multiple_of(own * W + x * 32, 32), 32), :]
        return send(11, ref, ref, across)

    def share_copy(d, n):
        if n == 0:
            ref = mi.at[pl.ds(pl.multiple_of(x * 256, 256), 256), :]
        else:
            ref = mof.at[pl.ds(pl.multiple_of(own * W + x * 32, 32), 32), :]
        return remote(ref, ref, x_send, x_recv.at[n], ((x + d) % 4 * 8 + s % 8, h))

    def w0_copy():
        return send(12, w0s, w0, across)

    @pl.when(home)
    def _():
        for c in range(PARTS):
            ring_k.give_a(c)
        mi[...] = m_in[...].astype(BF16)
        mof[col(own), :] = m_out[...].astype(BF16)
        mi_copy().start()
        mo_copy().start()
        share_m.start(0)

    @pl.when(away)
    def _():
        for c in range(PARTS):
            z_copy(0, c, kb, kf).start()

    query = dot(tok[...], wq[...]).astype(BF16)
    qb[...] = query
    value = dot(tok[...], wv[...]).astype(BF16)

    @pl.when(home)
    def _():
        mot[...] = m_out[...].T
        qf[:, col(h)] = query
        vf[:, col(h)] = value
        gates[g] = gown[...]

        def rows(c):
            r = pl.ds(pl.multiple_of(c * 32, 32), 32)
            return jnp.concatenate([m_in[r, :], mot[r, :]], axis=0)

        w0[...] = rows(g)
        w0s[...] = rows(g + 1 - 2 * z)
        w0_copy().start()

    @pl.when(away)
    def _():
        vb[...] = value
        gate_copy().start()

    def forward(c):
        pre = dot(kf[half(c), :], mi[...])
        sig = jax.nn.sigmoid(pre)
        hf[half(c), col(own)] = (pre * sig).astype(BF16)
        slope[half(c), :] = sig * (1.0 + pre * (1.0 - sig))
        share_h.start(c)

    @pl.when(home)
    def _():
        for c in range(PARTS):
            z_copy(0, c, kb, kf).wait_recv()
            ring_k.give_b(c)
        for c in range(PARTS):
            ring_k.relay(c)
        share_m.step(0)
        for c in range(PARTS):
            ring_v.give_a(c)
        for c in range(PARTS):
            ring_k.finish(c)
            side_rows(1, c, kf).start()
            forward(c)
        wait(vb, q_recv.at[2])
        for c in range(PARTS):
            ring_v.give_b(c)
        share_m.last(0)

    @pl.when(away)
    def _():
        for n, copy in enumerate((mi_copy, mo_copy)):
            copy().wait_recv()
            for d in (2, 1, 3):
                share_copy(d, n).start()
        for c in range(PARTS):
            z_copy(8, c, vb, vf).start()
        wait(mof.at[pl.ds(0, 96)], x_recv.at[1])
        share_m.start(0)
        wait(mi.at[pl.ds(0, 768)], x_recv.at[0])
        for c in range(PARTS):
            side_rows(1, c, kf).wait_recv()
            forward(c)
        share_m.step(0)
        for c in range(PARTS):
            z_copy(6, c, qb, qf).start()
        gate_copy().wait_recv()
        w0_copy().wait_recv()

    def send_gates(d, carry):
        remote(gates.at[g], gates.at[g], gt_send, gt_recv, group((g + d) % NS)).start()
        return carry

    lax.fori_loop(1, NS, send_gates, 0)
    for c in range(PARTS):
        share_h.step(c)

    @pl.when(home)
    def _():
        for c in range(PARTS):
            ring_v.relay(c)

    for c in range(PARTS):
        share_h.last(c)

    @pl.when(home)
    def _():
        for c in range(PARTS):
            ring_v.finish(c)
            side_rows(14, c, vf).start()

    @pl.when(away)
    def _():
        share_m.last(0)

    kt[...] = kf[...].T
    share_m.finish(0)

    @pl.when(away)
    def _():
        wait(vf, q_recv.at[8])

    for c in range(PARTS):
        share_h.finish(c)
        rf[half(c), :] = ((2.0 / T) * (dot(hf[half(c), :], mof[...]) - vf[half(c), :].astype(F32))).astype(BF16)

    @pl.when(home)
    def _():
        for c in range(PARTS):
            ring_q.give_a(c)

    rate = gates[g][2:3]
    g_out = dot(hf[:, col(own)].T, rf[...])
    gbuf[:, 32:64, :] = (g_out.T * -rate).astype(BF16).reshape(NS, 32, W)
    term = (dot(rf[...], mof[col(own), :], NT) * slope[...]).astype(BF16)
    gbuf[:, 0:32, :] = (dot(kt[...], term) * -rate).astype(BF16).reshape(NS, 32, W)

    def send_grad(d, carry):
        o = (g + d) % NS
        remote(gbuf.at[o], rbuf.at[g], a_send, a_recv.at[g], group(o)).start()
        return carry

    lax.fori_loop(1, NS, send_grad, 0)
    rbuf[g] = gbuf[g]

    def wo_copy(d):
        p = (h + d) % NH
        return remote(ao.at[:, col(p)], wo.at[pl.ds(pl.multiple_of(h * W, W), W), :], w_send, w_recv, (s, p))

    for d in range(1, NH):
        wo_copy(d).start()
    wo[pl.ds(pl.multiple_of(h * W, W), W), :] = ao[:, col(h)]

    pltpu.make_async_copy(gates.at[pl.ds(0, NS - 1)], gates.at[pl.ds(0, NS - 1)], gt_recv).wait()

    def step(c, carry):
        speed, weight = carry
        wbuf[c] = weight.astype(BF16)

        @pl.when(c != g)
        def _():
            remote(wbuf.at[c], wland.at[g], b_send, b_recv, group(c)).start()
            remote(gbuf.at[c], rbuf.at[c], a_send, a_recv.at[c], group(c)).wait_recv()

        gate = gates[c]
        speed = gate[0:1] * speed + rbuf[c].astype(F32)
        weight = gate[1:2] * weight + speed
        return speed, weight

    state = lax.fori_loop(0, 4, step, (jnp.zeros((64, W), F32), w0[...]))

    @pl.when(home)
    def _():
        wait(qb, q_recv.at[0])
        for c in range(PARTS):
            ring_q.give_b(c)

    state = lax.fori_loop(4, 20, step, state)

    @pl.when(home)
    def _():
        for c in range(PARTS):
            ring_q.relay(c)

    lax.fori_loop(20, NS, step, state)
    wland[g] = wbuf[g]
    @pl.when(home)
    def _():
        for c in range(PARTS):
            ring_q.finish(c)
            side_rows(7, c, qf).start()

    @pl.when(away)
    def _():
        wait(qf, q_recv.at[1])

    some = pl.ds(0, NS - 1)
    pltpu.make_async_copy(wland.at[some], wland.at[some], b_recv).wait()

    act = dot(qf[...], wland[:, 0:32, :].reshape(1024, W))
    hq[...] = (act * jax.nn.sigmoid(act)).astype(BF16)

    def part_two(c, b):
        return dot(hq[half(c), :], wland[pl.ds(b * 4, 4), 32:64, :].reshape(W, W), NT)

    sum_two = Sum(core, part_two, rs_out, rs_land, r_send, r_recv)
    sum_two.run()

    def t_copy(n, c, to):
        return send(n, tb.at[half(c)], tf.at[half(c), col(own)], to, c)

    for c in range(PARTS):
        rows_c = sum_two.last(c).astype(BF16)
        tb[half(c), :] = rows_c

        @pl.when(home)
        def _():
            t_copy(2, c, across).start()
            tf[half(c), col(own)] = rows_c
            ring_t.give_a(c)

        @pl.when(away)
        def _():
            t_copy(3, c, pair).start()
            t_copy(4, c, aside).start()

    @pl.when(home)
    def _():
        for c in range(PARTS):
            t_copy(4, c, aside).wait_recv()
            ring_t.give_b(c)

    @pl.when(away)
    def _():
        for c in range(PARTS):
            t_copy(2, c, across).wait_recv()
            ring_t.give_a(c)
            t_copy(3, c, pair).wait_recv()
            ring_t.give_b(c)

    for c in range(PARTS):
        ring_t.relay(c)
    zl = (s // 2) % 4

    def hop(c, n, slot, to_slot, to):
        r = pl.ds(c * (T // WINS), T // WINS)
        return remote(kv.at[slot, r], kv.at[to_slot, r], k_send.at[n], k_recv.at[c, to_slot], to)

    def own_copy(c, k):
        return hop(c, k, 0, 2 * k, (s + 2 * k, h))

    def side_copy(c):
        return hop(c, 0, 0, 1, (s + 1, h))

    def pass_copy(c, k):
        return hop(c, 4 + k, 2 * k, 2 * k + 1 - 2 * par, (s + 1 - 2 * par, h))

    def relay_copy(c, up):
        return hop(c, 9, 4, 6 if up else 2, (s + 2 if up else s - 2, h))

    def sends(k):
        ok = s + 2 * k < NS
        if k == 3:
            ok = ok & (zl != 0)
        if k == 1:
            ok = ok & (zl != 3)
        return ok

    def passes(k):
        return (s >= 2 * k) & ((par == 1) | (k < 4))

    for c in range(PARTS):
        ring_t.finish(c)
        for i in range(HALF // 128):
            r = slice(c * HALF + i * 128, c * HALF + (i + 1) * 128)
            rows_i = tf[r, :].astype(F32)
            mean = jnp.mean(rows_i * rows_i, axis=-1, keepdims=True)
            nrm[r, :] = (rows_i * lax.rsqrt(mean + EPS) * gain[...]).astype(BF16)
        kv[0, half(c), 0:W] = dot(nrm[half(c), :], ak[...]).astype(BF16)
        kv[0, half(c), W : 2 * W] = dot(nrm[half(c), :], av[...]).astype(BF16)
        if (c + 1) % (PARTS // WINS) == 0:
            w = (c + 1) // (PARTS // WINS) - 1
            for k in (2, 1, 3, 4):

                @pl.when(sends(k))
                def _():
                    own_copy(w, k).start()

            @pl.when(par == 0)
            def _():
                side_copy(w).start()

    query = dot(nrm[...], aq[...]).astype(BF16) * 0.125
    low = lax.broadcasted_iota(jnp.int32, (128, W), 1) < 64
    for i in range(4):
        part = query[i * 128 : (i + 1) * 128, :]
        qs[i, 0:128, :] = jnp.where(low, part, jnp.zeros_like(part))
        qs[i, 128:256, :] = jnp.where(low, jnp.zeros_like(part), part)
    m_s[...] = jnp.full_like(m_s, -1e30)
    acc[...] = jnp.zeros_like(acc)
    ones = jnp.ones((T, W), BF16)

    def attend(slot, mode, edge=None):
        values = jnp.concatenate([kv[slot, :, W : 2 * W], ones], axis=1)
        for i in range(4):
            sc = dot(qs[i], kv[slot, :, 0:W], NT)
            if mode != 1:
                iq = lax.broadcasted_iota(jnp.int32, (256, T), 0) % 128 + i * 128
                ik = lax.broadcasted_iota(jnp.int32, (256, T), 1)
                sc = jnp.where(iq >= ik if mode == 0 else ik - iq > edge, sc, -1e30)
            m_old = m_s[i]
            m_new = jnp.maximum(m_old, jnp.max(sc, axis=-1, keepdims=True))
            p = jnp.exp(sc - m_new)
            m_s[i] = m_new
            acc[i] = jnp.exp(m_old - m_new) * acc[i] + dot(p.astype(BF16), values)

    attend(0, 0)
    def arrive(c, slot):
        hop(c, 0, 0, slot, across).wait_recv()

    last = jnp.where(zl == 0, 1, 3)

    def chip(j):
        return jnp.where(j == 0, 2, jnp.where(j == 1, 4, jnp.where(j == 2, 4 - last, last)))

    def turn(j, carry):
        k = chip(j)
        odd = jnp.where(j == 0, par, 2 * chip(j - 1) - 1 + 2 * par)

        @pl.when((j < 4) & (s >= 2 * k))
        def _():
            for c in range(WINS):
                arrive(c, 2 * k)

                @pl.when((k == 2) & (zl == 2))
                def _():
                    relay_copy(c, True).start()

                @pl.when((k == 2) & (zl == 1))
                def _():
                    relay_copy(c, False).start()

                @pl.when(passes(k))
                def _():
                    pass_copy(c, k).start()

            attend(2 * k, 2, jnp.where(k == 4, 0, -2 * T))

        @pl.when((odd > 0) & (odd < 9) & (s >= odd))
        def _():
            for c in range(WINS):
                arrive(c, odd)
            attend(odd, 1)

        return carry

    lax.fori_loop(0, 5, turn, 0)
    for i in range(4):
        both = acc[i, :, 0:W] / acc[i, :, W : 2 * W]
        cf[i * 128 : (i + 1) * 128, col(h)] = jnp.where(low, both[0:128], both[128:256]).astype(BF16)

    def out_copy(c):
        return pltpu.make_async_copy(ob.at[half(c)], out_ref.at[half(c)], o_sem.at[c])

    def c_copy(c):
        ref = cf.at[half(c), col(h)]
        return send(5, ref, ref, across, c)

    for c in range(PARTS):
        c_copy(c).start()
        ring_c.give_a(c)
    for c in range(PARTS):
        c_copy(c).wait_recv()
        ring_c.give_b(c)
    wait(wo.at[pl.ds(0, 7 * W)], w_recv)
    for c in range(PARTS):
        ring_c.relay(c)
    for c in range(PARTS):
        ring_c.finish(c)
        ob[half(c), :] = dot(cf[half(c), :], wo[...]).astype(BF16)
        out_copy(c).start()

    @pl.when(home)
    def _():
        ring_k.drain()
        ring_q.drain()
        ring_v.drain()
        wait(vf, p_send.at[14])
        wait(kf, p_send.at[1])
        wait(qf, p_send.at[7])
        wait(tb, p_send.at[2])
        mi_copy().wait_send()
        mo_copy().wait_send()
        w0_copy().wait_send()

    @pl.when(away)
    def _():
        wait(kb, p_send.at[0])
        wait(qb, p_send.at[6])
        wait(tb, p_send.at[3])
        wait(tb, p_send.at[4])
        wait(vb, p_send.at[8])
        gate_copy().wait_send()
        wait(kf.at[pl.ds(0, 192)], x_send)

    ring_t.drain()
    ring_c.drain()
    wait(kb, p_send.at[5])
    for c in range(PARTS):
        out_copy(c).wait()
    for group_copies in (sum_two, share_h, share_m):
        group_copies.drain()
    wait(wo.at[pl.ds(0, 7 * W)], w_send)
    pltpu.make_async_copy(gates.at[some], gates.at[some], gt_send).wait()
    pltpu.make_async_copy(gbuf.at[some], gbuf.at[some], a_send).wait()
    pltpu.make_async_copy(wbuf.at[some], wbuf.at[some], b_send).wait()
    for k in range(1, 5):

        @pl.when(sends(k))
        def _():
            wait(kv.at[0], k_send.at[k])

        @pl.when(passes(k))
        def _():
            wait(kv.at[0], k_send.at[4 + k])

    @pl.when(par == 0)
    def _():
        wait(kv.at[0], k_send.at[0])

    @pl.when((s >= 4) & ((zl == 1) | (zl == 2)))
    def _():
        wait(kv.at[0], k_send.at[9])


def block(
    tokens, mem_query_w, mem_key_w, mem_value_w, mem_in, mem_out, forget_levels, momentum_levels, step_levels,
    plan, norm_gain, attn_query_w, attn_key_w, attn_value_w, attn_out_w,
):
    vm = pl.BlockSpec(memory_space=pltpu.VMEM)
    sm = pl.BlockSpec(memory_space=pltpu.SMEM)
    hb = pl.BlockSpec(memory_space=pl.ANY)
    V = pltpu.VMEM
    dma = pltpu.SemaphoreType.DMA
    big = V((T, 1024), BF16)
    slab = V((NS, 64, W), BF16)
    return pl.pallas_call(
        kernel,
        name="titans",
        out_shape=jax.ShapeDtypeStruct((T, W), BF16),
        in_specs=[hb] * 6 + [vm] * 3 + [sm, vm] + [hb] * 4,
        out_specs=hb,
        scratch_shapes=[
            big, V((1024, W), BF16), V((1024, W), BF16), V((1024, W), BF16), V((1024, W), F32), V((W, 1024), F32),
            V((1024, W), BF16), V((1024, W), BF16), V((1024, W), BF16), V((W, 1024), BF16), dma((10,)), V((T, W), BF16), dma((PARTS,)),
            big, big, big, big, big, big, big,
            V((1024, W), BF16), V((T, W), BF16), V((T, W), BF16), V((T, W), BF16), V((T, W), BF16),
            V((T, W), F32), V((T, W), BF16), V((1024, W), BF16), V((1024, 1024), BF16), V((1024, W), F32),
            V((64, W), F32), V((64, W), F32), V((1024, T), BF16),
            V((7, T, W), BF16), V((7, T, W), BF16), V((NS, 8, W), F32), V((8, W), F32),
            slab, slab, slab, slab,
            V((9, T, 2 * W), BF16), V((4, 256, W), BF16), big, V((4, 256, 1), F32), V((4, 256, 2 * W), F32),
            dma((5,)), dma((5, PARTS, 3)), dma, dma((1, 4)), dma, dma((PARTS, 4)), dma, dma((PARTS, 4)), dma((15,)), dma((6 * PARTS,)), dma((9,)),
            dma, dma, dma, dma,
            dma, dma((NS,)), dma, dma, dma((10,)), dma((WINS, 9)), dma, dma((2,)),
        ],
        compiler_params=pltpu.CompilerParams(collective_id=0, has_side_effects=True, vmem_limit_bytes=60 * 1024 * 1024),
    )(
        tokens, mem_query_w, mem_key_w, mem_value_w, mem_in, mem_out, forget_levels, momentum_levels, step_levels,
        plan, norm_gain.reshape(1, -1), attn_query_w, attn_key_w, attn_value_w, attn_out_w,
    )


def solution(mesh):
    seq, head = P("seq", None), P(None, "head")
    in_specs = (
        seq, head, head, head, head, P("head", None), head, head, head, P("seq"), P(), head, head, head, P("head", None),
    )
    return jax.shard_map(block, mesh=mesh, in_specs=in_specs, out_specs=P("seq", "head"), check_vma=False)
```

```python
import jax
import jax.numpy as jnp
from jax import lax
from jax.experimental import pallas as pl
from jax.experimental.pallas import tpu as pltpu
from jax.sharding import PartitionSpec as P

MESH = pl.DeviceIdType.MESH
F32 = jnp.float32
BF16 = jnp.bfloat16
EPS = 1e-06
NS = 32
NH = 8
T = 512
W = 128
NN = (((1,), (0,)), ((), ()))
NT = (((1,), (1,)), ((), ()))


def dot(a, b, dims=NN):
    return lax.dot_general(a, b, dims, preferred_element_type=F32)


def col(b):
    return pl.ds(pl.multiple_of(b * W, W), W)


def remote(src, dst, send, recv, device):
    return pltpu.make_async_remote_copy(
        src_ref=src, dst_ref=dst, send_sem=send, recv_sem=recv, device_id=device, device_id_type=MESH
    )


WINS = 2
PARTS = 4
HALF = T // PARTS


def half(c):
    return pl.ds(c * HALF, HALF)


def wait(ref, sem):
    pltpu.make_async_copy(ref, ref, sem).wait()


class Ring:
    def __init__(self, place, bit, buf, send, recv):
        self.s, self.y, self.z = place
        self.a, self.b = bit, 1 - bit
        self.buf, self.send, self.recv = buf, send, recv

    def copy(self, c, k):
        y, a, b = self.y, self.a, self.b
        up, down = (y + 1) % 4, (y + 3) % 4
        block, to = ((y * 2 + a, up), (y * 2 + a, down), (y * 2 + b, up), (y * 2 + b, down), (down * 2 + a, up), (up * 2 + b, down))[k]
        ref = self.buf.at[half(c), col(block)]
        return remote(ref, ref, self.send, self.recv.at[c, (0, 2, 2, 1, 2, 2)[k]], (self.s, to * 2 + self.z))

    def give_a(self, c):
        self.copy(c, 0).start()
        self.copy(c, 1).start()

    def give_b(self, c):
        self.copy(c, 2).start()
        self.copy(c, 3).start()

    def relay(self, c):
        self.copy(c, 0).wait_recv()
        self.copy(c, 4).start()
        self.copy(c, 3).wait_recv()
        self.copy(c, 5).start()

    def finish(self, c):
        wait(self.buf.at[half(c), pl.ds(0, 4 * W)], self.recv.at[c, 2])

    def drain(self):
        wait(self.buf.at[pl.ds(0, T * 6 // 8)], self.send)


class Core:
    def __init__(self, place):
        self.s, self.y, self.z = place
        self.k = self.s % 2
        up, down = (self.y + 1) % 4, (self.y + 3) % 4
        self.far = (self.y + 2) % 4
        self.next = jnp.where(self.k == 0, up, down)
        self.prev = jnp.where(self.k == 0, down, up)

    def at(self, y):
        return (self.s, y * 2 + self.z)

    def other(self):
        return (self.s + 1 - 2 * self.k, self.y * 2 + self.z)


class Share:
    def __init__(self, core, ref, four, seven, send, recv):
        self.me, self.ref, self.four, self.seven, self.send, self.recv = core, ref, four, seven, send, recv

    def copy(self, c, n):
        me = self.me
        y = (me.y, me.y, me.prev, me.y, me.prev, me.next, me.far)[n]
        to = (me.at(me.next), me.at(me.prev), me.at(me.next), me.other(), me.other(), me.other(), me.other())[n]
        ref = self.ref(c, y * 2 + me.k)
        return remote(ref, ref, self.send, self.recv.at[c, min(n, 3)], to)

    def start(self, c):
        for n in (0, 1, 3):
            self.copy(c, n).start()

    def step(self, c):
        self.copy(c, 0).wait_recv()
        self.copy(c, 2).start()
        self.copy(c, 4).start()
        self.copy(c, 1).wait_recv()
        self.copy(c, 5).start()

    def last(self, c):
        self.copy(c, 2).wait_recv()
        self.copy(c, 6).start()

    def finish(self, c):
        wait(self.four(c), self.recv.at[c, 3])

    def drain(self):
        wait(self.seven, self.send)


class Sum:
    def __init__(self, core, part, out, land, send, recv):
        self.me, self.part, self.out, self.land, self.send, self.recv = core, part, out, land, send, recv
        self.order = (core.far, core.next, core.prev, core.y)

    def copy(self, c, n):
        me = self.me
        to = me.other() if n < 4 else me.at(me.prev if n == 6 else me.next)
        return remote(self.out.at[n, half(c)], self.land.at[n, half(c)], self.send, self.recv.at[c, max(n - 3, 0)], to)

    def put(self, c, n, value):
        self.out[n, half(c), :] = value.astype(BF16)
        self.copy(c, n).start()

    def got(self, c, n):
        self.copy(c, n).wait_recv()
        return self.land[n, half(c), :].astype(F32)

    def give(self, c):
        for n, y in enumerate(self.order):
            self.put(c, n, self.part(c, y * 2 + 1 - self.me.k))

    def chip(self, c, n):
        return self.part(c, self.order[n] * 2 + self.me.k) + self.land[(0, 2, 1, 3)[n], half(c), :].astype(F32)

    def first(self, c):
        wait(self.land.at[pl.ds(0, 4), half(c)], self.recv.at[c, 0])
        self.put(c, 4, self.chip(c, 0))
        self.put(c, 6, self.chip(c, 2))

    def second(self, c):
        onward = self.chip(c, 1)
        self.put(c, 5, self.got(c, 4) + onward)

    def last(self, c):
        own = self.chip(c, 3)
        return own + self.got(c, 6) + self.got(c, 5)

    def run(self):
        for stage in (self.give, self.first, self.second):
            for c in range(PARTS):
                stage(c)

    def drain(self):
        wait(self.out, self.send)


def kernel(
    tok_h, wq_h, wk_h, wv_h, m_in_h, m_out_h, fg, mo, st, plan, gain, aq_h, ak_h, av_h, ao_h, out_ref,
    tok, wk, wq, wv, m_in, m_out, aq, ak, av, ao, l_sem, ob, o_sem,
    kf, qf, rf, tf, cf, hf, vf, wo, kb, qb, vb, tb, slope, hq, mi, mof, mot, w0, w0s, kt,
    rs_out, rs_land, gates, gown, gbuf, rbuf, wbuf, wland, kv, qs, nrm, m_s, acc,
    g_send, g_recv, f_send, f_recv, h_send, h_recv, r_send, r_recv, p_send, p_recv, q_recv, w_send, w_recv, gt_send, gt_recv,
    a_send, a_recv, b_send, b_recv, k_send, k_recv, x_send, x_recv,
):
    s, h = lax.axis_index("seq"), lax.axis_index("head")
    y, z = h // 2, h % 2
    place = (s, y, z)
    par = s % 2
    home = par == z
    away = par != z
    g = s - par + z
    core = Core(place)
    across = (s, y * 2 + 1 - z)
    aside = core.other()
    pair = (s + 1 - 2 * par, y * 2 + 1 - z)

    def group(c):
        return (c // 2 * 2 + par, y * 2 + c % 2)

    def send(n, src, dst, to, c=0):
        return remote(src, dst, p_send.at[n], p_recv.at[n * PARTS + c] if n < 6 else q_recv.at[n - 6], to)

    barrier = pltpu.get_barrier_semaphore()

    def greet_head(d, carry):
        pl.semaphore_signal(barrier, inc=1, device_id=(s, (h + d) % NH), device_id_type=MESH)
        return carry

    def greet_seq(d, carry):
        pl.semaphore_signal(barrier, inc=1, device_id=group((g + d) % NS), device_id_type=MESH)
        return carry

    lax.fori_loop(1, NH, greet_head, 0)
    lax.fori_loop(1, NS, greet_seq, 0)
    for to in (aside, pair):
        pl.semaphore_signal(barrier, inc=1, device_id=to, device_id_type=MESH)

    pairs = (
        (tok_h, tok), (wk_h, wk), (m_in_h, m_in), (m_out_h, m_out), (wq_h, wq), (wv_h, wv), (ao_h, ao), (ak_h, ak), (av_h, av), (aq_h, aq),
    )
    loads = [pltpu.make_async_copy(src, dst, l_sem.at[n]) for n, (src, dst) in enumerate(pairs)]
    for load in loads:
        load.start()
    loads[0].wait()
    loads[1].wait()
    key = dot(tok[...], wk[...]).astype(BF16)
    kb[...] = key

    @pl.when(home)
    def _():
        kf[:, col(h)] = key

    hot = lax.broadcasted_iota(jnp.int32, (16, W), 0) == plan[0]

    def row(table):
        return jnp.sum(jnp.where(hot, table[...], 0.0), axis=0, keepdims=True)

    gown[...] = jnp.concatenate([row(mo), 1.0 - row(fg), row(st), jnp.zeros((5, W), F32)], axis=0)
    pl.semaphore_wait(barrier, NH - 1 + NS - 1 + 2)

    for load in loads[2:]:
        load.wait()
    ring_k = Ring(place, z, kf, g_send.at[0], g_recv.at[0])
    ring_q = Ring(place, z, qf, g_send.at[1], g_recv.at[1])
    ring_t = Ring(place, par, tf, g_send.at[2], g_recv.at[2])
    ring_c = Ring(place, z, cf, g_send.at[3], g_recv.at[3])
    ring_v = Ring(place, z, vf, g_send.at[4], g_recv.at[4])
    own = y * 2 + par

    def cols_of(buf):
        return (lambda c, b: buf.at[half(c), col(b)], lambda c: buf.at[half(c), pl.ds(0, 4 * W)], buf.at[pl.ds(0, T * 7 // 8)])

    share_h = Share(core, *cols_of(hf), h_send, h_recv)
    share_m = Share(core, lambda c, b: mof.at[col(b)], lambda c: mof.at[pl.ds(0, 4 * W)], mof.at[pl.ds(0, 7 * W)], f_send, f_recv)

    x = s // 8

    def z_copy(n, c, src, dst):
        return send(n, src.at[half(c)], dst.at[half(c), col(h)], across, c)

    def side_rows(n, c, buf):
        return send(n, buf.at[half(c)], buf.at[half(c)], aside, c)

    def gate_copy():
        return send(13, gown, gates.at[s], pair)

    def mi_copy():
        ref = mi.at[pl.ds(pl.multiple_of(x * 256, 256), 256), :]
        return send(10, ref, ref, across)

    def mo_copy():
        ref = mof.at[pl.ds(pl.multiple_of(own * W + x * 32, 32), 32), :]
        return send(11, ref, ref, across)

    def share_copy(d, n):
        if n == 0:
            ref = mi.at[pl.ds(pl.multiple_of(x * 256, 256), 256), :]
        else:
            ref = mof.at[pl.ds(pl.multiple_of(own * W + x * 32, 32), 32), :]
        return remote(ref, ref, x_send, x_recv.at[n], ((x + d) % 4 * 8 + s % 8, h))

    def w0_copy():
        return send(12, w0s, w0, across)

    @pl.when(home)
    def _():
        for c in range(PARTS):
            ring_k.give_a(c)
        mi[...] = m_in[...].astype(BF16)
        mof[col(own), :] = m_out[...].astype(BF16)
        mi_copy().start()
        mo_copy().start()
        share_m.start(0)

    @pl.when(away)
    def _():
        for c in range(PARTS):
            z_copy(0, c, kb, kf).start()

    query = dot(tok[...], wq[...]).astype(BF16)
    qb[...] = query
    value = dot(tok[...], wv[...]).astype(BF16)

    @pl.when(home)
    def _():
        mot[...] = m_out[...].T
        qf[:, col(h)] = query
        vf[:, col(h)] = value
        gates[g] = gown[...]

        def rows(c):
            r = pl.ds(pl.multiple_of(c * 32, 32), 32)
            return jnp.concatenate([m_in[r, :], mot[r, :]], axis=0)

        w0[...] = rows(g)
        w0s[...] = rows(g + 1 - 2 * z)
        w0_copy().start()

    @pl.when(away)
    def _():
        vb[...] = value
        gate_copy().start()

    def forward(c):
        pre = dot(kf[half(c), :], mi[...])
        sig = jax.nn.sigmoid(pre)
        hf[half(c), col(own)] = (pre * sig).astype(BF16)
        slope[half(c), :] = sig * (1.0 + pre * (1.0 - sig))
        share_h.start(c)

    @pl.when(home)
    def _():
        for c in range(PARTS):
            z_copy(0, c, kb, kf).wait_recv()
            ring_k.give_b(c)
        for c in range(PARTS):
            ring_k.relay(c)
        share_m.step(0)
        for c in range(PARTS):
            ring_v.give_a(c)
        for c in range(PARTS):
            ring_k.finish(c)
            side_rows(1, c, kf).start()
            forward(c)
        wait(vb, q_recv.at[2])
        for c in range(PARTS):
            ring_v.give_b(c)
        share_m.last(0)

    @pl.when(away)
    def _():
        for n, copy in enumerate((mi_copy, mo_copy)):
            copy().wait_recv()
            for d in (2, 1, 3):
                share_copy(d, n).start()
        for c in range(PARTS):
            z_copy(8, c, vb, vf).start()
        wait(mof.at[pl.ds(0, 96)], x_recv.at[1])
        share_m.start(0)
        wait(mi.at[pl.ds(0, 768)], x_recv.at[0])
        for c in range(PARTS):
            side_rows(1, c, kf).wait_recv()
            forward(c)
        share_m.step(0)
        for c in range(PARTS):
            z_copy(6, c, qb, qf).start()
        gate_copy().wait_recv()
        w0_copy().wait_recv()

    def send_gates(d, carry):
        remote(gates.at[g], gates.at[g], gt_send, gt_recv, group((g + d) % NS)).start()
        return carry

    lax.fori_loop(1, NS, send_gates, 0)
    for c in range(PARTS):
        share_h.step(c)

    @pl.when(home)
    def _():
        for c in range(PARTS):
            ring_v.relay(c)

    for c in range(PARTS):
        share_h.last(c)

    @pl.when(home)
    def _():
        for c in range(PARTS):
            ring_v.finish(c)
            side_rows(14, c, vf).start()

    @pl.when(away)
    def _():
        share_m.last(0)

    kt[...] = kf[...].T
    share_m.finish(0)

    @pl.when(away)
    def _():
        wait(vf, q_recv.at[8])

    for c in range(PARTS):
        share_h.finish(c)
        rf[half(c), :] = ((2.0 / T) * (dot(hf[half(c), :], mof[...]) - vf[half(c), :].astype(F32))).astype(BF16)

    @pl.when(home)
    def _():
        for c in range(PARTS):
            ring_q.give_a(c)

    rate = gates[g][2:3]
    g_out = dot(hf[:, col(own)].T, rf[...])
    gbuf[:, 32:64, :] = (g_out.T * -rate).astype(BF16).reshape(NS, 32, W)
    term = (dot(rf[...], mof[col(own), :], NT) * slope[...]).astype(BF16)
    gbuf[:, 0:32, :] = (dot(kt[...], term) * -rate).astype(BF16).reshape(NS, 32, W)

    def send_grad(d, carry):
        o = (g + d) % NS
        remote(gbuf.at[o], rbuf.at[g], a_send, a_recv.at[g], group(o)).start()
        return carry

    lax.fori_loop(1, NS, send_grad, 0)
    rbuf[g] = gbuf[g]

    def wo_copy(d):
        p = (h + d) % NH
        return remote(ao.at[:, col(p)], wo.at[pl.ds(pl.multiple_of(h * W, W), W), :], w_send, w_recv, (s, p))

    for d in range(1, NH):
        wo_copy(d).start()
    wo[pl.ds(pl.multiple_of(h * W, W), W), :] = ao[:, col(h)]

    pltpu.make_async_copy(gates.at[pl.ds(0, NS - 1)], gates.at[pl.ds(0, NS - 1)], gt_recv).wait()

    def step(c, carry):
        speed, weight = carry
        wbuf[c] = weight.astype(BF16)

        @pl.when(c != g)
        def _():
            remote(wbuf.at[c], wland.at[g], b_send, b_recv, group(c)).start()
            remote(gbuf.at[c], rbuf.at[c], a_send, a_recv.at[c], group(c)).wait_recv()

        gate = gates[c]
        speed = gate[0:1] * speed + rbuf[c].astype(F32)
        weight = gate[1:2] * weight + speed
        return speed, weight

    state = lax.fori_loop(0, 4, step, (jnp.zeros((64, W), F32), w0[...]))

    @pl.when(home)
    def _():
        wait(qb, q_recv.at[0])
        for c in range(PARTS):
            ring_q.give_b(c)

    state = lax.fori_loop(4, 20, step, state)

    @pl.when(home)
    def _():
        for c in range(PARTS):
            ring_q.relay(c)

    lax.fori_loop(20, NS, step, state)
    wland[g] = wbuf[g]
    @pl.when(home)
    def _():
        for c in range(PARTS):
            ring_q.finish(c)
            side_rows(7, c, qf).start()

    @pl.when(away)
    def _():
        wait(qf, q_recv.at[1])

    some = pl.ds(0, NS - 1)
    pltpu.make_async_copy(wland.at[some], wland.at[some], b_recv).wait()

    act = dot(qf[...], wland[:, 0:32, :].reshape(1024, W))
    hq[...] = (act * jax.nn.sigmoid(act)).astype(BF16)

    def part_two(c, b):
        return dot(hq[half(c), :], wland[pl.ds(b * 4, 4), 32:64, :].reshape(W, W), NT)

    sum_two = Sum(core, part_two, rs_out, rs_land, r_send, r_recv)
    sum_two.run()

    def t_copy(n, c, to):
        return send(n, tb.at[half(c)], tf.at[half(c), col(own)], to, c)

    for c in range(PARTS):
        rows_c = sum_two.last(c).astype(BF16)
        tb[half(c), :] = rows_c

        @pl.when(home)
        def _():
            t_copy(2, c, across).start()
            tf[half(c), col(own)] = rows_c
            ring_t.give_a(c)

        @pl.when(away)
        def _():
            t_copy(3, c, pair).start()
            t_copy(4, c, aside).start()

    @pl.when(home)
    def _():
        for c in range(PARTS):
            t_copy(4, c, aside).wait_recv()
            ring_t.give_b(c)

    @pl.when(away)
    def _():
        for c in range(PARTS):
            t_copy(2, c, across).wait_recv()
            ring_t.give_a(c)
            t_copy(3, c, pair).wait_recv()
            ring_t.give_b(c)

    for c in range(PARTS):
        ring_t.relay(c)
    zl = (s // 2) % 4

    def hop(c, n, slot, to_slot, to):
        r = pl.ds(c * (T // WINS), T // WINS)
        return remote(kv.at[slot, r], kv.at[to_slot, r], k_send.at[n], k_recv.at[c, to_slot], to)

    def own_copy(c, k):
        return hop(c, k, 0, 2 * k, (s + 2 * k, h))

    def side_copy(c):
        return hop(c, 0, 0, 1, (s + 1, h))

    def pass_copy(c, k):
        return hop(c, 4 + k, 2 * k, 2 * k + 1 - 2 * par, (s + 1 - 2 * par, h))

    def relay_copy(c, up):
        return hop(c, 9, 4, 6 if up else 2, (s + 2 if up else s - 2, h))

    def sends(k):
        ok = s + 2 * k < NS
        if k == 3:
            ok = ok & (zl != 0)
        if k == 1:
            ok = ok & (zl != 3)
        return ok

    def passes(k):
        return (s >= 2 * k) & ((par == 1) | (k < 4))

    for c in range(PARTS):
        ring_t.finish(c)
        for i in range(HALF // 128):
            r = slice(c * HALF + i * 128, c * HALF + (i + 1) * 128)
            rows_i = tf[r, :].astype(F32)
            mean = jnp.mean(rows_i * rows_i, axis=-1, keepdims=True)
            nrm[r, :] = (rows_i * lax.rsqrt(mean + EPS) * gain[...]).astype(BF16)
        kv[0, half(c), 0:W] = dot(nrm[half(c), :], ak[...]).astype(BF16)
        kv[0, half(c), W : 2 * W] = dot(nrm[half(c), :], av[...]).astype(BF16)
        if (c + 1) % (PARTS // WINS) == 0:
            w = (c + 1) // (PARTS // WINS) - 1
            for k in (2, 4, 3, 1):

                @pl.when(sends(k))
                def _():
                    own_copy(w, k).start()

            @pl.when(par == 0)
            def _():
                side_copy(w).start()

    query = dot(nrm[...], aq[...]).astype(BF16) * 0.125
    low = lax.broadcasted_iota(jnp.int32, (128, W), 1) < 64
    for i in range(4):
        part = query[i * 128 : (i + 1) * 128, :]
        qs[i, 0:128, :] = jnp.where(low, part, jnp.zeros_like(part))
        qs[i, 128:256, :] = jnp.where(low, jnp.zeros_like(part), part)
    m_s[...] = jnp.full_like(m_s, -1e30)
    acc[...] = jnp.zeros_like(acc)
    ones = jnp.ones((T, W), BF16)

    def attend(slot, mode, edge=None):
        values = jnp.concatenate([kv[slot, :, W : 2 * W], ones], axis=1)
        for i in range(4):
            sc = dot(qs[i], kv[slot, :, 0:W], NT)
            if mode != 1:
                iq = lax.broadcasted_iota(jnp.int32, (256, T), 0) % 128 + i * 128
                ik = lax.broadcasted_iota(jnp.int32, (256, T), 1)
                sc = jnp.where(iq >= ik if mode == 0 else ik - iq > edge, sc, -1e30)
            m_old = m_s[i]
            m_new = jnp.maximum(m_old, jnp.max(sc, axis=-1, keepdims=True))
            p = jnp.exp(sc - m_new)
            m_s[i] = m_new
            acc[i] = jnp.exp(m_old - m_new) * acc[i] + dot(p.astype(BF16), values)

    attend(0, 0)
    def arrive(c, slot):
        hop(c, 0, 0, slot, across).wait_recv()

    last = jnp.where(zl == 0, 1, 3)

    def chip(j):
        return jnp.where(j == 0, 2, jnp.where(j == 1, 4, jnp.where(j == 2, 4 - last, last)))

    def turn(j, carry):
        k = chip(j)
        odd = jnp.where(j == 0, par, 2 * chip(j - 1) - 1 + 2 * par)

        @pl.when((j < 4) & (s >= 2 * k))
        def _():
            for c in range(WINS):
                arrive(c, 2 * k)

                @pl.when((k == 2) & (zl == 2))
                def _():
                    relay_copy(c, True).start()

                @pl.when((k == 2) & (zl == 1))
                def _():
                    relay_copy(c, False).start()

                @pl.when(passes(k))
                def _():
                    pass_copy(c, k).start()

            attend(2 * k, 2, jnp.where(k == 4, 0, -2 * T))

        @pl.when((odd > 0) & (odd < 9) & (s >= odd))
        def _():
            for c in range(WINS):
                arrive(c, odd)
            attend(odd, 1)

        return carry

    lax.fori_loop(0, 5, turn, 0)
    for i in range(4):
        both = acc[i, :, 0:W] / acc[i, :, W : 2 * W]
        cf[i * 128 : (i + 1) * 128, col(h)] = jnp.where(low, both[0:128], both[128:256]).astype(BF16)

    def out_copy(c):
        return pltpu.make_async_copy(ob.at[half(c)], out_ref.at[half(c)], o_sem.at[c])

    def c_copy(c):
        ref = cf.at[half(c), col(h)]
        return send(5, ref, ref, across, c)

    for c in range(PARTS):
        c_copy(c).start()
        ring_c.give_a(c)
    for c in range(PARTS):
        c_copy(c).wait_recv()
        ring_c.give_b(c)
    wait(wo.at[pl.ds(0, 7 * W)], w_recv)
    for c in range(PARTS):
        ring_c.relay(c)
    for c in range(PARTS):
        ring_c.finish(c)
        ob[half(c), :] = dot(cf[half(c), :], wo[...]).astype(BF16)
        out_copy(c).start()

    @pl.when(home)
    def _():
        ring_k.drain()
        ring_q.drain()
        ring_v.drain()
        wait(vf, p_send.at[14])
        wait(kf, p_send.at[1])
        wait(qf, p_send.at[7])
        wait(tb, p_send.at[2])
        mi_copy().wait_send()
        mo_copy().wait_send()
        w0_copy().wait_send()

    @pl.when(away)
    def _():
        wait(kb, p_send.at[0])
        wait(qb, p_send.at[6])
        wait(tb, p_send.at[3])
        wait(tb, p_send.at[4])
        wait(vb, p_send.at[8])
        gate_copy().wait_send()
        wait(kf.at[pl.ds(0, 192)], x_send)

    ring_t.drain()
    ring_c.drain()
    wait(kb, p_send.at[5])
    for c in range(PARTS):
        out_copy(c).wait()
    for group_copies in (sum_two, share_h, share_m):
        group_copies.drain()
    wait(wo.at[pl.ds(0, 7 * W)], w_send)
    pltpu.make_async_copy(gates.at[some], gates.at[some], gt_send).wait()
    pltpu.make_async_copy(gbuf.at[some], gbuf.at[some], a_send).wait()
    pltpu.make_async_copy(wbuf.at[some], wbuf.at[some], b_send).wait()
    for k in range(1, 5):

        @pl.when(sends(k))
        def _():
            wait(kv.at[0], k_send.at[k])

        @pl.when(passes(k))
        def _():
            wait(kv.at[0], k_send.at[4 + k])

    @pl.when(par == 0)
    def _():
        wait(kv.at[0], k_send.at[0])

    @pl.when((s >= 4) & ((zl == 1) | (zl == 2)))
    def _():
        wait(kv.at[0], k_send.at[9])


def block(
    tokens, mem_query_w, mem_key_w, mem_value_w, mem_in, mem_out, forget_levels, momentum_levels, step_levels,
    plan, norm_gain, attn_query_w, attn_key_w, attn_value_w, attn_out_w,
):
    vm = pl.BlockSpec(memory_space=pltpu.VMEM)
    sm = pl.BlockSpec(memory_space=pltpu.SMEM)
    hb = pl.BlockSpec(memory_space=pl.ANY)
    V = pltpu.VMEM
    dma = pltpu.SemaphoreType.DMA
    big = V((T, 1024), BF16)
    slab = V((NS, 64, W), BF16)
    return pl.pallas_call(
        kernel,
        name="titans",
        out_shape=jax.ShapeDtypeStruct((T, W), BF16),
        in_specs=[hb] * 6 + [vm] * 3 + [sm, vm] + [hb] * 4,
        out_specs=hb,
        scratch_shapes=[
            big, V((1024, W), BF16), V((1024, W), BF16), V((1024, W), BF16), V((1024, W), F32), V((W, 1024), F32),
            V((1024, W), BF16), V((1024, W), BF16), V((1024, W), BF16), V((W, 1024), BF16), dma((10,)), V((T, W), BF16), dma((PARTS,)),
            big, big, big, big, big, big, big,
            V((1024, W), BF16), V((T, W), BF16), V((T, W), BF16), V((T, W), BF16), V((T, W), BF16),
            V((T, W), F32), V((T, W), BF16), V((1024, W), BF16), V((1024, 1024), BF16), V((1024, W), F32),
            V((64, W), F32), V((64, W), F32), V((1024, T), BF16),
            V((7, T, W), BF16), V((7, T, W), BF16), V((NS, 8, W), F32), V((8, W), F32),
            slab, slab, slab, slab,
            V((9, T, 2 * W), BF16), V((4, 256, W), BF16), big, V((4, 256, 1), F32), V((4, 256, 2 * W), F32),
            dma((5,)), dma((5, PARTS, 3)), dma, dma((1, 4)), dma, dma((PARTS, 4)), dma, dma((PARTS, 4)), dma((15,)), dma((6 * PARTS,)), dma((9,)),
            dma, dma, dma, dma,
            dma, dma((NS,)), dma, dma, dma((10,)), dma((WINS, 9)), dma, dma((2,)),
        ],
        compiler_params=pltpu.CompilerParams(collective_id=0, has_side_effects=True, vmem_limit_bytes=60 * 1024 * 1024),
    )(
        tokens, mem_query_w, mem_key_w, mem_value_w, mem_in, mem_out, forget_levels, momentum_levels, step_levels,
        plan, norm_gain.reshape(1, -1), attn_query_w, attn_key_w, attn_value_w, attn_out_w,
    )


def solution(mesh):
    seq, head = P("seq", None), P(None, "head")
    in_specs = (
        seq, head, head, head, head, P("head", None), head, head, head, P("seq"), P(), head, head, head, P("head", None),
    )
    return jax.shard_map(block, mesh=mesh, in_specs=in_specs, out_specs=P("seq", "head"), check_vma=False)
```
